32 devices in a mesh: rep: 4 (over y, x), fsdp: 8 (over z, core).
Axes of the slice: x: 2, y: 2, z: 4, core: 2. Of those that a mesh axis runs over, the one named last changes fastest.
Arguments:
- latents: bfloat16 [8, 1024, 1152], P('fsdp', 'rep'), may hold values from -6 to 6
- condition: bfloat16 [8, 1152], P('fsdp'), may hold values from -6 to 6
- adapter_index: int32 [8, 5], P('fsdp'), may hold values from 0 to 7
- weight_mod: bfloat16 [1152, 6912], P('fsdp'), may hold values from -0.1875 to 0.1875
- weight_qkv: bfloat16 [1152, 3456], P('fsdp'), may hold values from -0.1875 to 0.1875
- weight_proj: bfloat16 [1152, 1152], P('fsdp'), may hold values from -3 to 3
- weight_fc1: bfloat16 [1152, 4608], P('fsdp'), may hold values from -0.1875 to 0.1875
- weight_fc2: bfloat16 [4608, 1152], P('fsdp'), may hold values from -0.09375 to 0.09375
- master: float32 [3391488], P('fsdp'), may hold values from -0.25 to 0.25
- moment1: float32 [3391488], P('fsdp'), may hold values from -64 to 64
- moment2: float32 [3391488], P('fsdp'), may hold values from 1 to 1000
- cotangent: bfloat16 [8, 1024, 1152], P('fsdp', 'rep'), may hold values from -6 to 6
Outputs:
- output: bfloat16 [8, 1024, 1152], P('fsdp', 'rep')
- latents_grad: float32 [8, 1024, 1152], P('fsdp', 'rep')
- condition_grad: float32 [8, 1152], P('fsdp')
- new_master: float32 [3391488], P('fsdp')
- new_moment1: float32 [3391488], P('fsdp')
- new_moment2: float32 [3391488], P('fsdp')
- rounded_adapters: bfloat16 [3391488], P('fsdp')
The draws below stay inside these ranges and needn't reach their ends.
All inputs are finite; a program needn't handle non-finite values.
Results may differ from the reference program's by a relative error of at most 0.03.
The reference program's roundings to bfloat16 on the way count: a program that leaves them out, or rounds other values in their place, can miss the bound.
Values may be sent and summed in bfloat16 or wider, within the bound.
A program may use at most 256 MiB of HBM per device.

```python
import math
import jax
import jax.numpy as jnp
from jax import lax

D = 1152
HEADS = 16
HEAD_DIM = 72
FF = 4608
RANK = 16
ADAPT = 8
LENGTH = 1024
STEP = 3
LATENTS = 8
P_SIZE = 3391488


def place_ends(entries, key, low, largest):
    shape = entries.shape
    spot = [jax.random.randint(jax.random.fold_in(key, axis), (), 0, shape[axis]) for axis in range(len(shape))]
    entries = entries.at[tuple(spot)].set(low)
    longest = shape.index(max(shape))
    spot[longest] = (spot[longest] + 1) % shape[longest]
    return entries.at[tuple(spot)].set(largest)


def level_of(own_key, shape, cuts, low, largest):
    loudness = 1.0
    for position, parts in cuts:
        draws = jax.random.uniform(jax.random.fold_in(jax.random.fold_in(own_key, 6), position), (parts,), jnp.float32, low / len(cuts), largest / len(cuts))
        loudness = loudness * jnp.repeat(jnp.exp(draws), shape[position] // parts).reshape((-1,) + (1,) * (len(shape) - 1 - position))
    return loudness


def noise(stream_key, dims, scale, reach, cuts=(), kind=jnp.bfloat16):
    values = scale * jax.random.normal(stream_key, dims, jnp.float32)
    if cuts:
        values = values * level_of(stream_key, dims, cuts, -0.22, 0.18)
    return jnp.clip(values, -reach, reach).astype(kind)


def setup_inputs(seed: int = 0) -> dict:
    key_of = jax.random.split(jax.random.key(seed), 13)
    latents = noise(key_of[0], (LATENTS, LENGTH, D), 1.0, 6.0, ((0, 8), (1, 4)))
    condition = noise(key_of[1], (LATENTS, D), 1.0, 6.0, ((0, 8),))
    adapter_index = place_ends(jax.random.randint(key_of[2], (LATENTS, 5), 0, ADAPT), jax.random.fold_in(key_of[2], 1), 0, ADAPT - 1).astype(jnp.int32)
    weight_mod = noise(key_of[3], (D, 6 * D), D ** -0.5, 0.1875, ((0, 8),))
    weight_qkv = noise(key_of[4], (D, 3 * D), D ** -0.5, 0.1875, ((0, 8),))
    weight_proj = noise(key_of[5], (D, D), (max(D // 256, 1)) ** -0.5, 3.0, ((0, 8),))
    weight_fc1 = noise(key_of[6], (D, FF), D ** -0.5, 0.1875, ((0, 8),))
    weight_fc2 = noise(key_of[7], (FF, D), FF ** -0.5, 0.09375, ((0, 8),))
    master = noise(key_of[8], (P_SIZE,), 0.04, 0.25, ((0, 8),), jnp.float32)
    moment1 = noise(key_of[9], (P_SIZE,), 10.0, 64.0, ((0, 8),), jnp.float32)
    moment2 = jnp.clip(jnp.exp(math.log(1000.0) - 6.9077553 * jax.random.uniform(key_of[10], (P_SIZE,), jnp.float32) ** level_of(key_of[10], (P_SIZE,), ((0, 8),), -0.2, 0.2)), 1.0, 1000.0)
    cotangent = noise(key_of[11], (LATENTS, LENGTH, D), 1.0, 6.0, ((0, 8), (1, 4)))
    return {"latents": latents, "condition": condition, "adapter_index": adapter_index, "weight_mod": weight_mod, "weight_qkv": weight_qkv, "weight_proj": weight_proj, "weight_fc1": weight_fc1, "weight_fc2": weight_fc2, "master": master, "moment1": moment1, "moment2": moment2, "cotangent": cotangent}


@jax.custom_vjp
def low(v):
    return lax.optimization_barrier(v.astype(jnp.bfloat16)).astype(jnp.float32)

@jax.custom_vjp
def low_back(v):
    return v

def low_keep(v):
    return (low(v), None)

def low_pass(kept, grad):
    return (grad,)

def back_keep(v):
    return (v, None)

def back_low(kept, grad):
    return (low(grad),)
low.defvjp(low_keep, low_pass)
low_back.defvjp(back_keep, back_low)
adapter_scale = 2.0
norm_eps = 1e-06

def both_low(v):
    return low(low_back(v))

def adapter_shapes():
    pairs = [(D, 6 * D), (D, 3 * D), (D, D), (D, FF), (FF, D)]
    shapes = []
    for fan_in, fan_out in pairs:
        shapes.append((ADAPT, fan_in, RANK))
        shapes.append((ADAPT, RANK, fan_out))
    return shapes

def unpack(flat):
    tables = []
    offset = 0
    for shape in adapter_shapes():
        count = shape[0] * shape[1] * shape[2]
        tables.append(flat[offset:offset + count].reshape(shape))
        offset = offset + count
    return tables

def layer_norm(values):
    centred = values - lax.optimization_barrier(jnp.mean(values, axis=-1, keepdims=True))
    spread = lax.optimization_barrier(jnp.mean(centred * centred, axis=-1, keepdims=True))
    return centred * lax.rsqrt(spread + norm_eps)

def block_forward(latent_rows, cond_rows, select, tables, frozen):
    maximal_precision = lax.Precision.HIGHEST
    modulation_weight, w_qkv, w_proj, w_fc1, w_fc2 = frozen
    groups, length, width = latent_rows.shape
    downs = [jnp.einsum('gk,kdr->gdr', select[:, selected_adapter], tables[2 * selected_adapter], precision=maximal_precision) for selected_adapter in range(5)]
    raise_factors = [jnp.einsum('gk,kro->gro', select[:, selected_adapter], tables[2 * selected_adapter + 1], precision=maximal_precision) for selected_adapter in range(5)]

    def project(rows, weight, selected_adapter):
        inner_lowrank = both_low(jnp.einsum('gtd,gdr->gtr', rows, downs[selected_adapter], precision=maximal_precision))
        additional_term = adapter_scale * jnp.einsum('dkj,dje->dke', inner_lowrank, raise_factors[selected_adapter], precision=maximal_precision)
        return jnp.einsum('gtd,de->gte', rows, weight, precision=maximal_precision) + additional_term
    condition_activated = low(jax.nn.silu(cond_rows))
    inner_modulation = low(jnp.einsum('gd,gdr->gr', condition_activated, downs[0], precision=maximal_precision))
    apply_modulation = jnp.dot(condition_activated, modulation_weight, precision=maximal_precision) + adapter_scale * jnp.einsum('si,siq->sq', inner_modulation, raise_factors[0], precision=maximal_precision)
    shift_a, scale_a, gate_a, shift_m, scale_m, gate_m = jnp.split(apply_modulation, 6, axis=1)
    first = low(layer_norm(latent_rows) * (1.0 + scale_a[:, None]) + shift_a[:, None])
    qkv = both_low(project(first, w_qkv, 1))
    query = qkv[..., :width].reshape(groups, length, HEADS, HEAD_DIM)
    keys = qkv[..., width:2 * width].reshape(groups, length, HEADS, HEAD_DIM)
    values = qkv[..., 2 * width:].reshape(groups, length, HEADS, HEAD_DIM)
    scores = low_back(jnp.einsum('gqhe,gkhe->ghqk', query, keys, precision=maximal_precision) * HEAD_DIM ** (-0.5))
    probs = jax.nn.softmax(scores, axis=-1)
    mixed = both_low(jnp.einsum('ghqk,gkhe->gqhe', low(probs), values, precision=maximal_precision).reshape(groups, length, width))
    attn_out = low_back(project(mixed, w_proj, 2))
    after_attn = latent_rows + gate_a[:, None] * attn_out
    second = low(layer_norm(after_attn) * (1.0 + scale_m[:, None]) + shift_m[:, None])
    pre = low_back(project(second, w_fc1, 3))
    act = low(jax.nn.gelu(pre, approximate=True))
    mlp_out = low_back(project(act, w_fc2, 4))
    return after_attn + gate_m[:, None] * mlp_out

def reference(latents, condition, adapter_index, weight_mod, weight_qkv, weight_proj, weight_fc1, weight_fc2, master, moment1, moment2, cotangent):
    frozen = [w.astype(jnp.float32) for w in (weight_mod, weight_qkv, weight_proj, weight_fc1, weight_fc2)]
    select = jax.nn.one_hot(adapter_index, ADAPT, dtype=jnp.float32)
    group = math.gcd(LATENTS, max(1, 4096 // LENGTH))

    def forward(latent_all, cond_all, flat):
        tables = unpack(low(flat))

        def one_group(packed):
            return block_forward(packed[0], packed[1], packed[2], tables, frozen)
        stacked = (latent_all.reshape(LATENTS // group, group, LENGTH, D), cond_all.reshape(LATENTS // group, group, D), select.reshape(LATENTS // group, group, 5, ADAPT))
        outs = lax.map(jax.checkpoint(one_group), stacked)
        return outs.reshape(LATENTS, LENGTH, D)
    result, pullback = jax.vjp(forward, latents.astype(jnp.float32), condition.astype(jnp.float32), master)
    latents_grad, condition_grad, grad = pullback(cotangent.astype(jnp.float32))
    new_moment1 = 0.5 * moment1 + 0.5 * grad
    new_moment2 = 0.5 * moment2 + 0.5 * grad * grad
    first_hat = new_moment1 / (1.0 - 0.5 ** STEP)
    second_hat = new_moment2 / (1.0 - 0.5 ** STEP)
    new_master = master - 0.01 * (first_hat / (jnp.sqrt(second_hat) + 1e-08) + 0.1 * master)
    return (result.astype(jnp.bfloat16), latents_grad, condition_grad, new_master, new_moment1, new_moment2, new_master.astype(jnp.bfloat16))
```

```python
import functools

import jax
import jax.numpy as jnp
from jax import lax
from jax.experimental import pallas as pl
from jax.experimental.pallas import tpu as pltpu
from jax.sharding import PartitionSpec as P

D = 1152
HEAD_DIM = 72
HEADS = 16
FF = 4608
RANK = 16
ADAPT = 8
STEP = 3
NORM_EPS = 1e-06
F32 = jnp.float32
BF16 = jnp.bfloat16
PAIRS = ((D, 6 * D), (D, 3 * D), (D, D), (D, FF), (FF, D))


def dot(a, b, dims, **kw):
    return lax.dot_general(a, b, (dims, ((), ())), preferred_element_type=F32, **kw)


def mm(a, b):
    return dot(a, b, ((1,), (0,)))


def mm_t(a, b):
    return dot(a, b, ((1,), (1,)))


def tmm(a, b):
    return dot(a, b, ((0,), (0,)))


def low(v):
    return v.astype(BF16)


def layer_norm(v):
    centred = v - jnp.mean(v, axis=-1, keepdims=True)
    inv = lax.rsqrt(jnp.mean(centred * centred, axis=-1, keepdims=True) + NORM_EPS)
    return centred * inv, inv


def layer_norm_back(g, normed, inv):
    m1 = jnp.mean(g, axis=-1, keepdims=True)
    m2 = jnp.mean(g * normed, axis=-1, keepdims=True)
    return inv * (g - m1 - normed * m2)


LANE = 128
GELU_C = 0.7978845608028654
GELU_A = 0.044715


def tile_sum(v):
    shift = LANE // 2
    while shift >= RANK:
        v = v + pltpu.roll(v, shift, 1)
        shift //= 2
    return v


def rep_copy(src, dst, send, recv, peer):
    return pltpu.make_async_remote_copy(src_ref=src, dst_ref=dst, send_sem=send, recv_sem=recv,
                                        device_id={"rep": peer}, device_id_type=pl.DeviceIdType.MESH)


def rep_barrier(R, r):
    sem = pltpu.get_barrier_semaphore()
    for i in range(1, R):
        pl.semaphore_signal(sem, inc=1, device_id={"rep": lax.rem(r + i, R)}, device_id_type=pl.DeviceIdType.MESH)
    pl.semaphore_wait(sem, R - 1)


def block(i, n):
    return pl.ds(pl.multiple_of(i * n, n), n)


def attn_fwd_kernel(R, hl, scale, lat_ref, dout_ref, mods_ref, wqkv_ref, z1_ref, bt1_ref, wproj_ref, z2_ref, bt2_ref,
                    h1_ref, u1_ref, qkv_ref, lse_ref, mixed_ref, u2_ref, ao_ref, x1_ref, h2a_ref, douta_ref,
                    wq, vt, osc, msend, mrecv, ds_sem, dr_sem, ms_sem, mr_sem, hs_sem, hr_sem):
    r = lax.axis_index("rep")
    T = dout_ref.shape[0]
    L = T * R
    cw = hl * HEAD_DIM
    rep_barrier(R, r)
    douta_ref[block(r, T), :] = dout_ref[...]

    def dcopy(i, who):
        return rep_copy(dout_ref, douta_ref.at[block(who, T)], ds_sem.at[i], dr_sem.at[who], lax.rem(r + i, R))

    for i in range(1, R):
        dcopy(i, r).start()
    wq[...] = jnp.zeros_like(wq)
    for i in range(3 * hl):
        wq[:, i * LANE:i * LANE + HEAD_DIM] = wqkv_ref[:, i * HEAD_DIM:(i + 1) * HEAD_DIM]
    shift_a, scale_a, gate_a = mods_ref[0:1, :], mods_ref[1:2, :], mods_ref[2:3, :]
    shift_m, scale_m = mods_ref[3:4, :], mods_ref[4:5, :]

    def first(c, _):
        rows = block(c, T)
        n, _ = layer_norm(lat_ref[rows, :].astype(F32))
        h1 = low(n * (1.0 + scale_a) + shift_a)
        h1_ref[rows, :] = h1
        u1 = low(tile_sum(mm(h1, z1_ref[...])))
        u1_ref[rows, :] = u1
        u1 = u1 * BF16(0.25)
        for j in range(3):
            cols = pl.ds(j * hl * LANE, hl * LANE)
            qkv_ref[rows, cols] = low(mm(h1, wq[:, cols]) + mm(u1, bt1_ref[:, cols]))
        return 0

    lax.fori_loop(0, R, first, 0)

    def transpose_v(h, _):
        vt[block(h, LANE), :] = qkv_ref[:, block(2 * hl + h, LANE)].T
        return 0

    lax.fori_loop(0, hl, transpose_v, 0)

    def mcopy(i, who):
        peer = lax.rem(r + i, R)
        return rep_copy(msend.at[block(peer, T)], mrecv.at[who], ms_sem.at[i], mr_sem.at[who], peer)

    def attend(i, _):
        peer = lax.rem(r + 1 + i, R)
        rows = block(peer, T)

        def head(h, _):
            s = mm_t(qkv_ref[:, block(hl + h, LANE)], qkv_ref[rows, block(h, LANE)])
            top = jnp.max(s, axis=0, keepdims=True)
            e = jnp.exp((s - top) * scale)
            total = jnp.sum(e, axis=0, keepdims=True)
            lse_ref[block(h, 8), rows] = jnp.broadcast_to(top * scale + jnp.log(total), (8, T))
            o = mm(vt[block(h, LANE), :], low(e * (1.0 / total)))
            osc[h] = o.T
            return 0

        lax.fori_loop(0, hl, head, 0)
        for h in range(hl):
            msend[rows, h * HEAD_DIM:(h + 1) * HEAD_DIM] = low(osc[h][:, :HEAD_DIM])

        @pl.when(i < R - 1)
        def _():
            mcopy(i + 1, r).start()
        return 0

    lax.fori_loop(0, R, attend, 0)
    mrecv[r] = msend[block(r, T), :]
    for i in range(1, R):
        mcopy(i, lax.rem(r + i, R)).wait_recv()
    for p in range(R):
        mixed_ref[:, p * cw:(p + 1) * cw] = mrecv[p]
    mixed = mixed_ref[...]
    u2 = low(tile_sum(mm(mixed, z2_ref[...])))
    u2_ref[...] = u2
    ao = mm(mixed, wproj_ref[...]) + mm(u2 * BF16(0.25), bt2_ref[...])
    ao_ref[...] = ao
    x1 = lat_ref[block(r, T), :].astype(F32) + gate_a * ao
    x1_ref[...] = x1
    n, _ = layer_norm(x1)
    h2a_ref[block(r, T), :] = low(n * (1.0 + scale_m) + shift_m)

    def hcopy(i, who):
        return rep_copy(h2a_ref.at[block(r, T)], h2a_ref.at[block(who, T)], hs_sem.at[i], hr_sem.at[who], lax.rem(r + i, R))

    for i in range(1, R):
        hcopy(i, r).start()
    for i in range(1, R):
        p = lax.rem(r + i, R)
        hcopy(i, p).wait_recv()
        dcopy(i, p).wait_recv()
        dcopy(i, r).wait_send()
        mcopy(i, r).wait_send()
        hcopy(i, r).wait_send()


def mlp_kernel(R, h2a_ref, douta_ref, mods_ref, w1_ref, z3_ref, bt3_ref, w2_ref, z4_ref, bt4_ref, x1_ref,
               out_ref, dx1_ref, dmod_ref, da3_ref, db3_ref, da4_ref, db4_ref,
               act, gp, u3s, u4s, du4s, du3s, dpre, psend, precv, pown, gsend, grecv, gown,
               ps_sem, pr_sem, gs_sem, gr_sem):
    r = lax.axis_index("rep")
    T = x1_ref.shape[0]
    rep_barrier(R, r)
    scale_m, gate_m = mods_ref[4:5, :], mods_ref[5:6, :]

    def pcopy(i, who):
        peer = lax.rem(r + i, R)
        return rep_copy(psend.at[block(peer, T)], precv.at[who], ps_sem.at[i], pr_sem.at[who], peer)

    def gcopy(i, who):
        peer = lax.rem(r + i, R)
        return rep_copy(gsend.at[block(peer, T)], grecv.at[who], gs_sem.at[i], gr_sem.at[who], peer)

    def forward(i, _):
        peer = lax.rem(r + 1 + i, R)
        rows = block(peer, T)
        h2 = h2a_ref[rows, :]
        u3 = low(tile_sum(mm(h2, z3_ref[...])))
        u3s[rows, :] = u3
        x = mm(h2, w1_ref[...]) + mm(u3 * BF16(0.25), bt3_ref[...])
        x2 = x * x
        t = jnp.tanh(GELU_C * (x + GELU_A * x * x2))
        a = low(0.5 * x * (1.0 + t))
        act[rows, :] = a
        gp[rows, :] = 0.5 * (1.0 + t) + 0.5 * x * (1.0 - t * t) * (GELU_C * (1.0 + 3.0 * GELU_A * x2))
        u4 = low(tile_sum(mm(a, z4_ref[...])))
        u4s[rows, :] = u4
        part = mm(a, w2_ref[...]) + mm(u4 * BF16(0.25), bt4_ref[...])
        psend[rows, :] = low(part)
        pown[...] = part

        @pl.when(i < R - 1)
        def _():
            pcopy(i + 1, r).start()
        return 0

    lax.fori_loop(0, R, forward, 0)

    def backward(i, _):
        peer = lax.rem(r + 1 + i, R)
        rows = block(peer, T)
        dm = low(douta_ref[rows, :].astype(F32) * gate_m)
        douta_ref[rows, :] = dm
        du4 = low(2.0 * mm_t(dm, bt4_ref[...]))
        du4s[rows, :] = du4
        d_act = mm_t(dm, w2_ref[...]) + mm_t(du4, z4_ref[...])
        dp = low(d_act * gp[rows, :])
        dpre[rows, :] = dp
        du3 = low(2.0 * mm_t(dp, bt3_ref[...]))
        du3s[rows, :] = du3
        part = mm_t(dp, w1_ref[...]) + mm_t(du3, z3_ref[...])
        gsend[rows, :] = low(part)
        gown[...] = part

        @pl.when(i < R - 1)
        def _():
            gcopy(i + 1, r).start()
        return 0

    dout = douta_ref[block(r, T), :].astype(F32)
    lax.fori_loop(0, R, backward, 0)
    da4_ref[...] = tmm(du4s[...], act[...])[:RANK]
    db4_ref[...] = 2.0 * tmm(u4s[...], douta_ref[...])[:RANK]
    da3_ref[...] = tmm(du3s[...], h2a_ref[...])[:RANK]
    db3_ref[...] = 2.0 * tmm(u3s[...], dpre[...])[:RANK]
    mlp = pown[...]
    for i in range(1, R):
        p = lax.rem(r + i, R)
        pcopy(i, p).wait_recv()
        mlp = mlp + precv[p].astype(F32)
    x1 = x1_ref[...]
    out_ref[...] = low(x1 + gate_m * mlp)
    dmod_ref[...] = jnp.zeros_like(dmod_ref)
    dmod_ref[2:3, :] = jnp.sum(dout * mlp, axis=0, keepdims=True)
    n2, inv2 = layer_norm(x1)
    dh2 = gown[...]
    for i in range(1, R):
        p = lax.rem(r + i, R)
        gcopy(i, p).wait_recv()
        dh2 = dh2 + grecv[p].astype(F32)
    dmod_ref[0:1, :] = jnp.sum(dh2, axis=0, keepdims=True)
    dmod_ref[1:2, :] = jnp.sum(dh2 * n2, axis=0, keepdims=True)
    dx1_ref[...] = dout + layer_norm_back(dh2 * (1.0 + scale_m), n2, inv2)
    for i in range(1, R):
        pcopy(i, r).wait_send()
        gcopy(i, r).wait_send()


def attn_bwd_kernel(R, hl, scale, dx1_ref, ao_ref, mods_ref, wproj_ref, z2_ref, bt2_ref, mixed_ref, u2_ref,
                    qkv_ref, lse_ref, wqkv_ref, z1_ref, bt1_ref, h1_ref, u1_ref, lat_ref,
                    lg_ref, dmod_ref, da2_ref, db2_ref, da1_ref, db1_ref,
                    wq, kt, msend, mrecv, mpad, dkv, dqkv, du1s, gsend, grecv, gown,
                    ms_sem, mr_sem, gs_sem, gr_sem):
    r = lax.axis_index("rep")
    T = dx1_ref.shape[0]
    cw = hl * HEAD_DIM
    rep_barrier(R, r)
    scale_a, gate_a = mods_ref[1:2, :], mods_ref[2:3, :]
    dx1 = dx1_ref[...]
    dmod_ref[...] = jnp.zeros_like(dmod_ref)
    dmod_ref[2:3, :] = jnp.sum(dx1 * ao_ref[...], axis=0, keepdims=True)
    da = low(dx1 * gate_a)
    du2 = low(2.0 * mm_t(da, bt2_ref[...]))
    dm = low(mm_t(da, wproj_ref[...]) + mm_t(du2, z2_ref[...]))
    for p in range(R):
        msend[p] = dm[:, p * cw:(p + 1) * cw]

    def mcopy(i, who):
        peer = lax.rem(r + i, R)
        return rep_copy(msend.at[peer], mrecv.at[who], ms_sem.at[i], mr_sem.at[who], peer)

    for i in range(1, R):
        mcopy(i, r).start()
    mrecv[r] = msend[r]
    db2_ref[...] = 2.0 * tmm(u2_ref[...], da)[:RANK]
    da2_ref[...] = tmm(du2, mixed_ref[...])[:RANK]
    wq[...] = jnp.zeros_like(wq)
    for i in range(3 * hl):
        wq[:, i * LANE:i * LANE + HEAD_DIM] = wqkv_ref[:, i * HEAD_DIM:(i + 1) * HEAD_DIM]

    def transpose_k(h, _):
        kt[block(h, LANE), :] = qkv_ref[:, block(hl + h, LANE)].T
        return 0

    lax.fori_loop(0, hl, transpose_k, 0)
    dkv[...] = jnp.zeros_like(dkv)
    mpad[...] = jnp.zeros_like(mpad)

    def attend(i, _):
        p = lax.rem(r + i, R)

        @pl.when(i > 0)
        def _():
            mcopy(i, p).wait_recv()
        for h in range(hl):
            mpad[h, :, :HEAD_DIM] = mrecv[p][:, h * HEAD_DIM:(h + 1) * HEAD_DIM]
        rows = block(p, T)

        def head(h, _):
            q = qkv_ref[rows, block(h, LANE)]
            g = mpad[h]
            s = mm_t(qkv_ref[:, block(hl + h, LANE)], q)
            lse = lse_ref[block(h, 8), rows][0:1, :]
            probs = jnp.exp(s * scale - lse)
            dkv[:, block(hl + h, LANE)] += mm(low(probs), g)
            dp = mm_t(qkv_ref[:, block(2 * hl + h, LANE)], g)
            centre = jnp.sum(probs * dp, axis=0, keepdims=True)
            ds = low(probs * (dp - centre))
            dkv[:, block(h, LANE)] += mm(ds, q)
            dq = mm(kt[block(h, LANE), :], ds)
            dqkv[rows, block(h, LANE)] = low(dq.T * scale)
            return 0

        lax.fori_loop(0, hl, head, 0)
        return 0

    lax.fori_loop(0, R, attend, 0)

    def gcopy(i, who):
        peer = lax.rem(r + i, R)
        return rep_copy(gsend.at[block(peer, T)], grecv.at[who], gs_sem.at[i], gr_sem.at[who], peer)

    def backward(i, _):
        peer = lax.rem(r + 1 + i, R)
        rows = block(peer, T)
        dqkv[rows, hl * LANE:2 * hl * LANE] = low(dkv[rows, :hl * LANE] * scale)
        dqkv[rows, 2 * hl * LANE:] = low(dkv[rows, hl * LANE:])
        g = dqkv[rows, :]
        du1 = low(2.0 * mm_t(g, bt1_ref[...]))
        du1s[rows, :] = du1
        part = mm_t(g, wq[...]) + mm_t(du1, z1_ref[...])
        gsend[rows, :] = low(part)
        gown[...] = part

        @pl.when(i < R - 1)
        def _():
            gcopy(i + 1, r).start()
        return 0

    lax.fori_loop(0, R, backward, 0)
    da1_ref[...] = tmm(du1s[...], h1_ref[...])[:RANK]
    db1_ref[...] = 2.0 * tmm(u1_ref[...], dqkv[...])[:RANK]
    n1, inv1 = layer_norm(lat_ref[...].astype(F32))
    dh1 = gown[...]
    for i in range(1, R):
        p = lax.rem(r + i, R)
        gcopy(i, p).wait_recv()
        dh1 = dh1 + grecv[p].astype(F32)
    dmod_ref[0:1, :] = jnp.sum(dh1, axis=0, keepdims=True)
    dmod_ref[1:2, :] = jnp.sum(dh1 * n1, axis=0, keepdims=True)
    lg_ref[...] = dx1_ref[...] + layer_norm_back(dh1 * (1.0 + scale_a), n1, inv1)
    for i in range(1, R):
        mcopy(i, r).wait_send()
        gcopy(i, r).wait_send()


def sds(shape, dtype):
    return jax.ShapeDtypeStruct(shape, dtype)


def dma(n):
    return pltpu.SemaphoreType.DMA((n,))


def call(body, cid, out_shape, scratch, *args):
    vm = pl.BlockSpec(memory_space=pltpu.VMEM)
    return pl.pallas_call(body, out_shape=out_shape, in_specs=[vm] * len(args), out_specs=[vm] * len(out_shape),
                          scratch_shapes=scratch,
                          compiler_params=pltpu.CompilerParams(collective_id=cid, has_side_effects=True,
                                                               vmem_limit_bytes=63 * 2 ** 20))(*args)


def spread_down(a):
    n = a.shape[0]
    keep = (jnp.arange(n) % 8)[:, None] == (jnp.arange(LANE) // RANK)[None, :]
    return jnp.where(keep, jnp.tile(a, (1, 8)), jnp.zeros((), a.dtype))


def shards(latents, condition, adapter_index, weight_mod, weight_qkv, weight_proj, weight_fc1, weight_fc2,
           master, moment1, moment2, cotangent):
    R = lax.axis_size("rep")
    F = lax.axis_size("fsdp")
    r = lax.axis_index("rep")
    f = lax.axis_index("fsdp")
    T = latents.shape[1]
    L = T * R
    hl = HEADS // R
    cw = hl * HEAD_DIM
    fw = FF // (F * R)
    rows = weight_qkv.shape[0]
    scale = HEAD_DIM ** -0.5

    def gather(x, axis_name, axis=0):
        return lax.all_gather(x, axis_name, axis=axis, tiled=True)

    def pick(x, axis):
        return lax.dynamic_index_in_dim(x, r, axis, keepdims=False)

    wqkv = gather(pick(weight_qkv.reshape(rows, 3, R, cw), 2).reshape(rows, 3 * cw), "fsdp")
    wproj = gather(weight_proj, "fsdp")
    w1 = gather(pick(weight_fc1.reshape(rows, F, R, fw), 2).reshape(rows, F * fw), "fsdp")
    w2 = gather(pick(weight_fc2.reshape(R, fw, D), 0), "fsdp")
    flat = gather(master.astype(BF16), "fsdp")
    A, B = [], []
    off = 0
    for j, (a, b) in enumerate(PAIRS):
        n = a * RANK
        A.append(lax.dynamic_slice(flat, (off + adapter_index[0, j] * n,), (n,)).reshape(a, RANK))
        off += ADAPT * n
        n = b * RANK
        B.append(lax.dynamic_slice(flat, (off + adapter_index[0, j] * n,), (n,)).reshape(RANK, b))
        off += ADAPT * n
    B1 = jnp.pad(pick(B[1].reshape(RANK, 3, R, hl, HEAD_DIM), 2), ((0, 0), (0, 0), (0, 0), (0, LANE - HEAD_DIM)))
    B1 = B1.reshape(RANK, 3 * hl * LANE)
    B3 = pick(B[3].reshape(RANK, F, R, fw), 2).reshape(RANK, F * fw)
    A4 = pick(A[4].reshape(F, R, fw, RANK), 1).reshape(F * fw, RANK)
    bt1, bt2, bt3, bt4 = [jnp.tile(x, (8, 1)) for x in (B1, B[2], B3, B[4])]
    z1, z2, z3, z4 = [spread_down(x) for x in (A[1], A[2], A[3], A4)]

    cond = condition.astype(F32)
    sig = jax.nn.sigmoid(cond)
    cs = low(cond * sig)
    cs_all = gather(cs, "fsdp")
    cs_mine = lax.dynamic_slice(cs_all, (0, f * rows), (F, rows))
    mod = lax.psum_scatter(mm(cs_mine, weight_mod), "fsdp", scatter_dimension=0, tiled=True)
    u0 = low(mm(cs, A[0]))
    mod = mod + 2.0 * mm(u0, B[0])
    mods = jnp.pad(mod.reshape(6, D), ((0, 2), (0, 0)))

    lat_all = gather(latents[0], "rep")
    FW = F * fw
    W3 = 3 * hl * LANE
    h1, u1, qkv, lse, mixed, u2, ao, x1, h2a, douta = call(
        functools.partial(attn_fwd_kernel, R, hl, scale), 1,
        [sds((L, D), BF16), sds((L, LANE), BF16), sds((L, W3), BF16), sds((hl * 8, L), F32), sds((T, D), BF16),
         sds((T, LANE), BF16), sds((T, D), F32), sds((T, D), F32), sds((L, D), BF16), sds((L, D), BF16)],
        [pltpu.VMEM((D, W3), BF16), pltpu.VMEM((hl * LANE, L), BF16), pltpu.VMEM((hl, T, LANE), F32),
         pltpu.VMEM((L, cw), BF16), pltpu.VMEM((R, T, cw), BF16)] + [dma(R)] * 6,
        lat_all, cotangent[0], mods, wqkv, z1, bt1, wproj, z2, bt2)
    out, dx1, dmod_m, dA3, dB3, dA4, dB4 = call(
        functools.partial(mlp_kernel, R), 2,
        [sds((T, D), BF16), sds((T, D), F32), sds((8, D), F32), sds((RANK, D), F32), sds((RANK, FW), F32),
         sds((RANK, FW), F32), sds((RANK, D), F32)],
        [pltpu.VMEM((L, FW), BF16), pltpu.VMEM((L, FW), F32)] + [pltpu.VMEM((L, LANE), BF16)] * 4
        + [pltpu.VMEM((L, FW), BF16)]
        + [pltpu.VMEM((L, D), BF16), pltpu.VMEM((R, T, D), BF16), pltpu.VMEM((T, D), F32)] * 2 + [dma(R)] * 4,
        h2a, douta, mods, w1, z3, bt3, w2, z4, bt4, x1)
    lg, dmod_a, dA2, dB2, dA1, dB1 = call(
        functools.partial(attn_bwd_kernel, R, hl, scale), 3,
        [sds((T, D), F32), sds((8, D), F32), sds((RANK, D), F32), sds((RANK, D), F32), sds((RANK, D), F32),
         sds((RANK, W3), F32)],
        [pltpu.VMEM((D, W3), BF16), pltpu.VMEM((hl * LANE, L), BF16), pltpu.VMEM((R, T, cw), BF16),
         pltpu.VMEM((R, T, cw), BF16), pltpu.VMEM((hl, T, LANE), BF16), pltpu.VMEM((L, 2 * hl * LANE), F32),
         pltpu.VMEM((L, W3), BF16), pltpu.VMEM((L, LANE), BF16), pltpu.VMEM((L, D), BF16), pltpu.VMEM((R, T, D), BF16),
         pltpu.VMEM((T, D), F32)] + [dma(R)] * 4,
        dx1, ao, mods, wproj, z2, bt2, mixed, u2, qkv, lse, wqkv, z1, bt1, h1, u1, latents[0])
    hi = dict(precision=lax.Precision.HIGHEST)
    d_mod = jnp.concatenate([dmod_a[0:3], dmod_m[0:3]], axis=0).reshape(1, 6 * D)
    d_mod = lax.psum(d_mod, "rep")
    du0 = 2.0 * dot(d_mod, B[0].astype(F32), ((1,), (1,)), **hi)
    dB0 = 2.0 * tmm(u0.astype(F32), d_mod)
    dA0 = tmm(cs.astype(F32), du0)
    d_mod_all = gather(d_mod, "fsdp")
    d_cs = dot(d_mod_all, weight_mod.astype(F32), ((1,), (1,)), **hi)
    d_cs = lax.all_to_all(d_cs, "fsdp", split_axis=0, concat_axis=1, tiled=True)
    d_cs = d_cs + dot(du0, A[0].astype(F32), ((1,), (1,)), **hi)
    condition_grad = d_cs * (sig * (1.0 + cond * (1.0 - sig)))
    one = (r == 0).astype(F32)

    def spread(x, shape, axis):
        full = jnp.zeros(shape, F32)
        return lax.dynamic_update_slice_in_dim(full, jnp.expand_dims(x, axis), r, axis)

    dB1 = dB1.reshape(RANK, 3, hl, LANE)[..., :HEAD_DIM].reshape(RANK, 3, cw)
    dB1f = spread(dB1, (RANK, 3, R, cw), 2)
    dB3f = spread(dB3.reshape(RANK, F, fw), (RANK, F, R, fw), 2)
    dA4f = spread(dA4.T.reshape(F, fw, RANK), (F, R, fw, RANK), 1)
    full = [dA0 * one, dB0 * one, dA1.T, dB1f, dA2.T, dB2, dA3.T, dB3f, dA4f, dB4]
    pieces = []
    for i, g in enumerate(full):
        sel = jax.nn.one_hot(adapter_index[0, i // 2], ADAPT, dtype=F32)
        pieces.append((sel[:, None] * g.reshape(1, -1)).reshape(-1))
    grad = lax.psum_scatter(jnp.concatenate(pieces).astype(BF16), "fsdp", scatter_dimension=0, tiled=True).astype(F32)
    grad = lax.psum(grad, "rep")
    nm1 = 0.5 * moment1 + 0.5 * grad
    nm2 = 0.5 * moment2 + 0.5 * grad * grad
    c = 1.0 - 0.5 ** STEP
    nm = master - 0.01 * ((nm1 / c) / (jnp.sqrt(nm2 / c) + 1e-08) + 0.1 * master)
    return (out[None], lg[None], condition_grad, nm, nm1, nm2, nm.astype(BF16))


def solution(mesh):
    tok = P("fsdp", "rep", None)
    row = P("fsdp", None)
    vec = P("fsdp")
    return jax.shard_map(shards, mesh=mesh,
                         in_specs=(tok, row, row, row, row, row, row, row, vec, vec, vec, tok),
                         out_specs=(tok, tok, row, vec, vec, vec, vec), check_vma=False)
```

```python
import functools

import jax
import jax.numpy as jnp
from jax import lax
from jax.experimental import pallas as pl
from jax.experimental.pallas import tpu as pltpu
from jax.sharding import PartitionSpec as P

D = 1152
HEAD_DIM = 72
HEADS = 16
FF = 4608
RANK = 16
ADAPT = 8
STEP = 3
NORM_EPS = 1e-06
F32 = jnp.float32
BF16 = jnp.bfloat16
PAIRS = ((D, 6 * D), (D, 3 * D), (D, D), (D, FF), (FF, D))


def dot(a, b, dims, **kw):
    return lax.dot_general(a, b, (dims, ((), ())), preferred_element_type=F32, **kw)


def mm(a, b):
    return dot(a, b, ((1,), (0,)))


def mm_t(a, b):
    return dot(a, b, ((1,), (1,)))


def tmm(a, b):
    return dot(a, b, ((0,), (0,)))


def low(v):
    return v.astype(BF16)


def layer_norm(v):
    centred = v - jnp.mean(v, axis=-1, keepdims=True)
    inv = lax.rsqrt(jnp.mean(centred * centred, axis=-1, keepdims=True) + NORM_EPS)
    return centred * inv, inv


def layer_norm_back(g, normed, inv):
    m1 = jnp.mean(g, axis=-1, keepdims=True)
    m2 = jnp.mean(g * normed, axis=-1, keepdims=True)
    return inv * (g - m1 - normed * m2)


LANE = 128
GELU_C = 0.7978845608028654
GELU_A = 0.044715


def tile_sum(v):
    shift = LANE // 2
    while shift >= RANK:
        v = v + pltpu.roll(v, shift, 1)
        shift //= 2
    return v


def rep_copy(src, dst, send, recv, peer):
    return pltpu.make_async_remote_copy(src_ref=src, dst_ref=dst, send_sem=send, recv_sem=recv,
                                        device_id={"rep": peer}, device_id_type=pl.DeviceIdType.MESH)


def rep_barrier(R, r):
    sem = pltpu.get_barrier_semaphore()
    for i in range(1, R):
        pl.semaphore_signal(sem, inc=1, device_id={"rep": lax.rem(r + i, R)}, device_id_type=pl.DeviceIdType.MESH)
    pl.semaphore_wait(sem, R - 1)


def block(i, n):
    return pl.ds(pl.multiple_of(i * n, n), n)


def attn_fwd_kernel(R, hl, scale, lat_ref, dout_ref, mods_ref, wqkv_ref, z1_ref, bt1_ref, wproj_ref, z2_ref, bt2_ref,
                    h1_ref, u1_ref, qkv_ref, lse_ref, mixed_ref, u2_ref, ao_ref, x1_ref, h2a_ref, douta_ref,
                    wq, vt, osc, msend, mrecv, ds_sem, dr_sem, ms_sem, mr_sem, hs_sem, hr_sem):
    r = lax.axis_index("rep")
    T = dout_ref.shape[0]
    L = T * R
    cw = hl * HEAD_DIM
    rep_barrier(R, r)
    douta_ref[block(r, T), :] = dout_ref[...]

    def dcopy(i, who):
        return rep_copy(dout_ref, douta_ref.at[block(who, T)], ds_sem.at[i], dr_sem.at[who], lax.rem(r + i, R))

    for i in range(1, R):
        dcopy(i, r).start()
    wq[...] = jnp.zeros_like(wq)
    for i in range(3 * hl):
        wq[:, i * LANE:i * LANE + HEAD_DIM] = wqkv_ref[:, i * HEAD_DIM:(i + 1) * HEAD_DIM]
    shift_a, scale_a, gate_a = mods_ref[0:1, :], mods_ref[1:2, :], mods_ref[2:3, :]
    shift_m, scale_m = mods_ref[3:4, :], mods_ref[4:5, :]

    def first(c, _):
        rows = block(c, T)
        n, _ = layer_norm(lat_ref[rows, :].astype(F32))
        h1 = low(n * (1.0 + scale_a) + shift_a)
        h1_ref[rows, :] = h1
        u1 = low(tile_sum(mm(h1, z1_ref[...])))
        u1_ref[rows, :] = u1
        u1 = u1 * BF16(0.25)
        for j in range(3):
            cols = pl.ds(j * hl * LANE, hl * LANE)
            qkv_ref[rows, cols] = low(mm(h1, wq[:, cols]) + mm(u1, bt1_ref[:, cols]))
        return 0

    lax.fori_loop(0, R, first, 0)

    def transpose_v(h, _):
        vt[block(h, LANE), :] = qkv_ref[:, block(2 * hl + h, LANE)].T
        return 0

    lax.fori_loop(0, hl, transpose_v, 0)

    def mcopy(i, who):
        peer = lax.rem(r + i, R)
        return rep_copy(msend.at[block(peer, T)], mrecv.at[who], ms_sem.at[i], mr_sem.at[who], peer)

    def attend(i, _):
        peer = lax.rem(r + 1 + i, R)
        rows = block(peer, T)

        def head(h, _):
            s = mm_t(qkv_ref[:, block(hl + h, LANE)], qkv_ref[rows, block(h, LANE)])
            top = jnp.max(s, axis=0, keepdims=True)
            e = jnp.exp((s - top) * scale)
            total = jnp.sum(e, axis=0, keepdims=True)
            lse_ref[block(h, 8), rows] = jnp.broadcast_to(top * scale + jnp.log(total), (8, T))
            o = mm(vt[block(h, LANE), :], low(e * (1.0 / total)))
            osc[h] = o.T
            return 0

        lax.fori_loop(0, hl, head, 0)
        for h in range(hl):
            msend[rows, h * HEAD_DIM:(h + 1) * HEAD_DIM] = low(osc[h][:, :HEAD_DIM])

        @pl.when(i < R - 1)
        def _():
            mcopy(i + 1, r).start()
        return 0

    lax.fori_loop(0, R, attend, 0)
    mrecv[r] = msend[block(r, T), :]
    for i in range(1, R):
        mcopy(i, lax.rem(r + i, R)).wait_recv()
    for p in range(R):
        mixed_ref[:, p * cw:(p + 1) * cw] = mrecv[p]
    mixed = mixed_ref[...]
    u2 = low(tile_sum(mm(mixed, z2_ref[...])))
    u2_ref[...] = u2
    ao = mm(mixed, wproj_ref[...]) + mm(u2 * BF16(0.25), bt2_ref[...])
    ao_ref[...] = ao
    x1 = lat_ref[block(r, T), :].astype(F32) + gate_a * ao
    x1_ref[...] = x1
    n, _ = layer_norm(x1)
    h2a_ref[block(r, T), :] = low(n * (1.0 + scale_m) + shift_m)

    def hcopy(i, who):
        return rep_copy(h2a_ref.at[block(r, T)], h2a_ref.at[block(who, T)], hs_sem.at[i], hr_sem.at[who], lax.rem(r + i, R))

    for i in range(1, R):
        hcopy(i, r).start()
    for i in range(1, R):
        p = lax.rem(r + i, R)
        hcopy(i, p).wait_recv()
        dcopy(i, p).wait_recv()
        dcopy(i, r).wait_send()
        mcopy(i, r).wait_send()
        hcopy(i, r).wait_send()


def mlp_kernel(R, h2a_ref, douta_ref, mods_ref, w1_ref, z3_ref, bt3_ref, w2_ref, z4_ref, bt4_ref, x1_ref,
               out_ref, dx1_ref, dmod_ref, da3_ref, db3_ref, da4_ref, db4_ref,
               act, gp, u3s, u4s, du4s, du3s, dpre, psend, precv, pown, gsend, grecv, gown,
               ps_sem, pr_sem, gs_sem, gr_sem):
    r = lax.axis_index("rep")
    T = x1_ref.shape[0]
    rep_barrier(R, r)
    scale_m, gate_m = mods_ref[4:5, :], mods_ref[5:6, :]

    def pcopy(i, who):
        peer = lax.rem(r + i, R)
        return rep_copy(psend.at[block(peer, T)], precv.at[who], ps_sem.at[i], pr_sem.at[who], peer)

    def gcopy(i, who):
        peer = lax.rem(r + i, R)
        return rep_copy(gsend.at[block(peer, T)], grecv.at[who], gs_sem.at[i], gr_sem.at[who], peer)

    def forward(i, _):
        peer = lax.rem(r + 1 + i, R)
        rows = block(peer, T)
        h2 = h2a_ref[rows, :]
        u3 = low(tile_sum(mm(h2, z3_ref[...])))
        u3s[rows, :] = u3
        x = mm(h2, w1_ref[...]) + mm(u3 * BF16(0.25), bt3_ref[...])
        x2 = x * x
        t = jnp.tanh(GELU_C * (x + GELU_A * x * x2))
        a = low(0.5 * x * (1.0 + t))
        act[rows, :] = a
        gp[rows, :] = 0.5 * (1.0 + t) + 0.5 * x * (1.0 - t * t) * (GELU_C * (1.0 + 3.0 * GELU_A * x2))
        u4 = low(tile_sum(mm(a, z4_ref[...])))
        u4s[rows, :] = u4
        part = mm(a, w2_ref[...]) + mm(u4 * BF16(0.25), bt4_ref[...])
        psend[rows, :] = low(part)
        pown[...] = part

        @pl.when(i < R - 1)
        def _():
            pcopy(i + 1, r).start()
        return 0

    lax.fori_loop(0, R, forward, 0)

    def backward(i, _):
        peer = lax.rem(r + 1 + i, R)
        rows = block(peer, T)
        dm = low(douta_ref[rows, :].astype(F32) * gate_m)
        douta_ref[rows, :] = dm
        du4 = low(2.0 * mm_t(dm, bt4_ref[...]))
        du4s[rows, :] = du4
        d_act = mm_t(dm, w2_ref[...]) + mm_t(du4, z4_ref[...])
        dp = low(d_act * gp[rows, :])
        dpre[rows, :] = dp
        du3 = low(2.0 * mm_t(dp, bt3_ref[...]))
        du3s[rows, :] = du3
        part = mm_t(dp, w1_ref[...]) + mm_t(du3, z3_ref[...])
        gsend[rows, :] = low(part)
        gown[...] = part

        @pl.when(i < R - 1)
        def _():
            gcopy(i + 1, r).start()
        return 0

    dout = douta_ref[block(r, T), :].astype(F32)
    lax.fori_loop(0, R, backward, 0)
    da4_ref[...] = tmm(du4s[...], act[...])[:RANK]
    db4_ref[...] = 2.0 * tmm(u4s[...], douta_ref[...])[:RANK]
    da3_ref[...] = tmm(du3s[...], h2a_ref[...])[:RANK]
    db3_ref[...] = 2.0 * tmm(u3s[...], dpre[...])[:RANK]
    mlp = pown[...]
    for i in range(1, R):
        p = lax.rem(r + i, R)
        pcopy(i, p).wait_recv()
        mlp = mlp + precv[p].astype(F32)
    x1 = x1_ref[...]
    out_ref[...] = low(x1 + gate_m * mlp)
    dmod_ref[...] = jnp.zeros_like(dmod_ref)
    dmod_ref[2:3, :] = jnp.sum(dout * mlp, axis=0, keepdims=True)
    n2, inv2 = layer_norm(x1)
    dh2 = gown[...]
    for i in range(1, R):
        p = lax.rem(r + i, R)
        gcopy(i, p).wait_recv()
        dh2 = dh2 + grecv[p].astype(F32)
    dmod_ref[0:1, :] = jnp.sum(dh2, axis=0, keepdims=True)
    dmod_ref[1:2, :] = jnp.sum(dh2 * n2, axis=0, keepdims=True)
    dx1_ref[...] = dout + layer_norm_back(dh2 * (1.0 + scale_m), n2, inv2)
    for i in range(1, R):
        pcopy(i, r).wait_send()
        gcopy(i, r).wait_send()


def attn_bwd_kernel(R, hl, scale, dx1_ref, ao_ref, mods_ref, wproj_ref, z2_ref, bt2_ref, mixed_ref, u2_ref,
                    qkv_ref, lse_ref, wqkv_ref, z1_ref, bt1_ref, h1_ref, u1_ref, lat_ref,
                    lg_ref, dmod_ref, da2_ref, db2_ref, da1_ref, db1_ref,
                    wq, kt, msend, mrecv, mpad, dkv, dqkv, du1s, gsend, grecv, gown,
                    ms_sem, mr_sem, gs_sem, gr_sem):
    r = lax.axis_index("rep")
    T = dx1_ref.shape[0]
    cw = hl * HEAD_DIM
    rep_barrier(R, r)
    scale_a, gate_a = mods_ref[1:2, :], mods_ref[2:3, :]
    dx1 = dx1_ref[...]
    dmod_ref[...] = jnp.zeros_like(dmod_ref)
    dmod_ref[2:3, :] = jnp.sum(dx1 * ao_ref[...], axis=0, keepdims=True)
    da = low(dx1 * gate_a)
    du2 = low(2.0 * mm_t(da, bt2_ref[...]))
    dm = low(mm_t(da, wproj_ref[...]) + mm_t(du2, z2_ref[...]))
    for p in range(R):
        msend[p] = dm[:, p * cw:(p + 1) * cw]

    def mcopy(i, who):
        peer = lax.rem(r + i, R)
        return rep_copy(msend.at[peer], mrecv.at[who], ms_sem.at[i], mr_sem.at[who], peer)

    for i in range(1, R):
        mcopy(i, r).start()
    mrecv[r] = msend[r]
    db2_ref[...] = 2.0 * tmm(u2_ref[...], da)[:RANK]
    da2_ref[...] = tmm(du2, mixed_ref[...])[:RANK]
    wq[...] = jnp.zeros_like(wq)
    for i in range(3 * hl):
        wq[:, i * LANE:i * LANE + HEAD_DIM] = wqkv_ref[:, i * HEAD_DIM:(i + 1) * HEAD_DIM]

    def transpose_k(h, _):
        kt[block(h, LANE), :] = qkv_ref[:, block(hl + h, LANE)].T
        return 0

    lax.fori_loop(0, hl, transpose_k, 0)
    dkv[...] = jnp.zeros_like(dkv)
    mpad[...] = jnp.zeros_like(mpad)

    def attend(i, _):
        p = lax.rem(r + i, R)

        @pl.when(i > 0)
        def _():
            mcopy(i, p).wait_recv()
        for h in range(hl):
            mpad[h, :, :HEAD_DIM] = mrecv[p][:, h * HEAD_DIM:(h + 1) * HEAD_DIM]
        rows = block(p, T)

        def head(h, _):
            q = qkv_ref[rows, block(h, LANE)]
            g = mpad[h]
            s = mm_t(qkv_ref[:, block(hl + h, LANE)], q)
            lse = lse_ref[block(h, 8), rows][0:1, :]
            probs = jnp.exp(s * scale - lse)
            dkv[:, block(hl + h, LANE)] += mm(low(probs), g)
            dp = mm_t(qkv_ref[:, block(2 * hl + h, LANE)], g)
            centre = jnp.sum(probs * dp, axis=0, keepdims=True)
            ds = low(probs * (dp - centre))
            dkv[:, block(h, LANE)] += mm(ds, q)
            dq = mm(kt[block(h, LANE), :], ds)
            dqkv[rows, block(h, LANE)] = low(dq.T * scale)
            return 0

        lax.fori_loop(0, hl, head, 0)
        return 0

    lax.fori_loop(0, R, attend, 0)

    def gcopy(i, who):
        peer = lax.rem(r + i, R)
        return rep_copy(gsend.at[block(peer, T)], grecv.at[who], gs_sem.at[i], gr_sem.at[who], peer)

    def backward(i, _):
        peer = lax.rem(r + 1 + i, R)
        rows = block(peer, T)
        dqkv[rows, hl * LANE:2 * hl * LANE] = low(dkv[rows, :hl * LANE] * scale)
        dqkv[rows, 2 * hl * LANE:] = low(dkv[rows, hl * LANE:])
        g = dqkv[rows, :]
        du1 = low(2.0 * mm_t(g, bt1_ref[...]))
        du1s[rows, :] = du1
        part = mm_t(g, wq[...]) + mm_t(du1, z1_ref[...])
        gsend[rows, :] = low(part)
        gown[...] = part

        @pl.when(i < R - 1)
        def _():
            gcopy(i + 1, r).start()
        return 0

    lax.fori_loop(0, R, backward, 0)
    da1_ref[...] = tmm(du1s[...], h1_ref[...])[:RANK]
    db1_ref[...] = 2.0 * tmm(u1_ref[...], dqkv[...])[:RANK]
    n1, inv1 = layer_norm(lat_ref[...].astype(F32))
    dh1 = gown[...]
    for i in range(1, R):
        p = lax.rem(r + i, R)
        gcopy(i, p).wait_recv()
        dh1 = dh1 + grecv[p].astype(F32)
    dmod_ref[0:1, :] = jnp.sum(dh1, axis=0, keepdims=True)
    dmod_ref[1:2, :] = jnp.sum(dh1 * n1, axis=0, keepdims=True)
    lg_ref[...] = dx1_ref[...] + layer_norm_back(dh1 * (1.0 + scale_a), n1, inv1)
    for i in range(1, R):
        mcopy(i, r).wait_send()
        gcopy(i, r).wait_send()


def sds(shape, dtype):
    return jax.ShapeDtypeStruct(shape, dtype)


def dma(n):
    return pltpu.SemaphoreType.DMA((n,))


def call(body, cid, out_shape, scratch, *args):
    vm = pl.BlockSpec(memory_space=pltpu.VMEM)
    return pl.pallas_call(body, out_shape=out_shape, in_specs=[vm] * len(args), out_specs=[vm] * len(out_shape),
                          scratch_shapes=scratch,
                          compiler_params=pltpu.CompilerParams(collective_id=cid, has_side_effects=True,
                                                               vmem_limit_bytes=63 * 2 ** 20))(*args)


PARTS = 4
UNIT_COUNT = 23
TABLES = (1, 6, 1, 3, 1, 1, 1, 4, 4, 1)


class Layout:
    def __init__(self, F):
        self.F = F
        self.n = [t * F // 8 for t in TABLES]
        self.first = [ADAPT * sum(self.n[:j]) for j in range(11)]
        self.slot = [sum(self.n[:j]) for j in range(11)]
        self.slots = self.slot[10]
        self.rows = D // F
        self.part = self.rows // PARTS
        self.lo, self.hi = [], []
        for f in range(F):
            held = [self.slot_of(g) for g in range(UNIT_COUNT * f, UNIT_COUNT * (f + 1))]
            self.lo.append(min(held))
            self.hi.append(max(held) + 1)
        self.most = max(h - l for h, l in zip(self.hi, self.lo))
        self.flat_row = [s * self.rows for s in self.slot]

    def slot_of(self, g):
        j = max(j for j in range(10) if self.first[j] <= g)
        return self.slot[j] + (g - self.first[j]) % self.n[j]

    def low_of(self, f):
        lo = self.lo[0] + 0 * f
        for i in range(1, self.F):
            lo = jnp.where(f == i, self.lo[i], lo)
        return lo

    def find(self, g):
        j, a, s = 0 * g, g // self.n[0], g % self.n[0]
        for t in range(1, 10):
            here = g >= self.first[t]
            rest = g - self.first[t]
            j = jnp.where(here, t // 2, j)
            a = jnp.where(here, rest // self.n[t], a)
            s = jnp.where(here, self.slot[t] + rest % self.n[t], s)
        return j, a, s


def fsdp_copy(src, dst, send, recv, peer):
    return pltpu.make_async_remote_copy(src_ref=src, dst_ref=dst, send_sem=send, recv_sem=recv,
                                        device_id={"fsdp": peer}, device_id_type=pl.DeviceIdType.MESH)


def full_barrier(R, r, F, f):
    sem = pltpu.get_barrier_semaphore()
    for i in range(1, R):
        pl.semaphore_signal(sem, inc=1, device_id={"rep": lax.rem(r + i, R)}, device_id_type=pl.DeviceIdType.MESH)
    for i in range(1, F):
        pl.semaphore_signal(sem, inc=1, device_id={"fsdp": lax.rem(f + i, F)}, device_id_type=pl.DeviceIdType.MESH)
    pl.semaphore_wait(sem, R + F - 2)


def iota(shape, axis):
    return lax.broadcasted_iota(jnp.int32, shape, axis)


def front_kernel(R, lay, hl, lat_ref, msg_ref, wmod_ref, units_ref, cs_ref,
                 lata_ref, idx_ref, mods_ref, u0c_ref, b0_ref, z0_ref,
                 z1_ref, bt1_ref, z2_ref, bt2_ref, z3_ref, bt3_ref, z4_ref, bt4_ref,
                 sel, sbuf, rbuf, parts, flat, msend, mrecv, wide, pad1, a4s,
                 ls_sem, lr_sem, is_sem, ir_sem, ss_sem, sr_sem, ms_sem, mr_sem, as_sem, ar_sem):
    F, Q, UQ, UR = lay.F, PARTS, lay.part, lay.rows
    r = lax.axis_index("rep")
    f = lax.axis_index("fsdp")
    T = lat_ref.shape[0]
    rows = wmod_ref.shape[0]
    fw = FF // (F * R)
    full_barrier(R, r, F, f)

    def icopy(i, who):
        peer = lax.rem(f + i, F)
        return fsdp_copy(msg_ref.at[peer], idx_ref.at[who], is_sem.at[i], ir_sem.at[who], peer)

    def lcopy(i, who):
        return rep_copy(lat_ref, lata_ref.at[block(who, T)], ls_sem.at[i], lr_sem.at[who], lax.rem(r + i, R))

    def over_fsdp(step):
        def one(i, _):
            step(i)
            return 0

        lax.fori_loop(1, F, one, 0)

    over_fsdp(lambda i: icopy(i, f).start())
    for i in range(1, R):
        lcopy(i, r).start()
    idx_ref[f] = msg_ref[f]
    lata_ref[block(r, T), :] = lat_ref[...]
    sel[...] = jnp.where(iota((D, D // 8), 0) // 8 == iota((D, D // 8), 1), 1.0, 0.0).astype(BF16)
    sbuf[...] = jnp.zeros_like(sbuf)
    over_fsdp(lambda i: icopy(i, lax.rem(f + i, F)).wait_recv())
    lo = lay.low_of(f)

    def choose(u, _):
        j, a, s = lay.find(f * UNIT_COUNT + u)
        unit = units_ref[u]

        def each(l, _):
            hit = idx_ref[l, pl.ds(1 + j, 1), :][:, :LANE] == a.astype(F32)
            sbuf[l, s - lo] = low(jnp.where(hit, unit, sbuf[l, s - lo].astype(F32)))
            return 0

        return lax.fori_loop(0, F, each, 0)

    lax.fori_loop(0, UNIT_COUNT, choose, 0)

    def scopy(i, who, n):
        peer = lax.rem(f + i, F)
        return fsdp_copy(sbuf.at[peer, pl.ds(0, n)], rbuf.at[who, pl.ds(0, n)], ss_sem.at[i], sr_sem.at[who], peer)

    width = [h - l for h, l in zip(lay.hi, lay.lo)]
    for owner in range(F):
        @pl.when((f == owner) & (r < Q))
        def _():
            over_fsdp(lambda i: scopy(i, f, width[owner]).start())
    rbuf[f] = sbuf[f]
    chosen = low(jnp.concatenate([idx_ref[l, 0:1, :rows] for l in range(F)], axis=0))
    for j in range(6):
        part = mm(chosen, wmod_ref[:, j * D:(j + 1) * D])
        for l in range(F):
            msend[l, j:j + 1, :] = part[l:l + 1, :]

    def mcopy(i, who):
        peer = lax.rem(f + i, F)
        return fsdp_copy(msend.at[peer], mrecv.at[who], ms_sem.at[i], mr_sem.at[who], peer)

    over_fsdp(lambda i: mcopy(i, f).start())
    mrecv[f] = msend[f]

    def acopy(i, who):
        return rep_copy(parts.at[r], parts.at[who], as_sem.at[i], ar_sem.at[who], lax.rem(r + i, R))

    @pl.when(r < Q)
    def _():
        for owner in range(F):
            @pl.when(f != owner)
            def _():
                scopy(lax.rem(owner - f + F, F), owner, width[owner]).wait_recv()
        for s in range(lay.slots):
            held = [o for o in range(F) if lay.lo[o] <= s < lay.hi[o]]
            total = rbuf[held[0], s - lay.lo[held[0]]].astype(F32)
            for o in held[1:]:
                total = total + rbuf[o, s - lay.lo[o]].astype(F32)
            parts[r, s] = low(total)
        for i in range(1, R):
            acopy(i, r).start()

    def arrived(q):
        @pl.when(r != q)
        def _():
            acopy(lax.rem(q - r + R, R), q).wait_recv()

    for q in range(Q):
        arrived(q)

        def unpack(s, _):
            flat[pl.ds(s * UR + q * UQ, UQ), :] = parts[q, s].astype(F32)
            return 0

        lax.fori_loop(0, lay.slots, unpack, 0)

    keep = iota((D, LANE), 1) // RANK == iota((D, LANE), 0) % 8

    def spread(x):
        n = x.shape[0]
        return low(jnp.where(keep[:8 * n], mm(sel[:8 * n, :n], low(x)), 0.0))

    def cols(j, c):
        nb = PAIRS[j][1] // LANE
        return flat[pl.ds(lay.flat_row[2 * j + 1] + c, RANK, stride=nb), :]

    def tiled(x):
        return jnp.concatenate([low(x)] * 8, axis=0)

    def a_rows(j):
        return flat[lay.flat_row[2 * j]:lay.flat_row[2 * j] + D // 8, :]

    z0_ref[...] = spread(a_rows(0))
    z1_ref[...] = spread(a_rows(1))
    z2_ref[...] = spread(a_rows(2))
    z3_ref[...] = spread(a_rows(3))
    fwl = F * fw
    if fw % 8 == 0:
        for i in range(F):
            for k in range(R):
                @pl.when(r == k)
                def _():
                    at = lay.flat_row[8] + (i * (FF // F) + k * fw) // 8
                    a4s[i * fw // 8:(i + 1) * fw // 8, :] = flat[at:at + fw // 8, :]
        z4_ref[...] = spread(a4s[...])
    else:
        for b in range(FF // D):
            at = lay.flat_row[8] + b * D // 8
            a4s[fwl + b * D:fwl + (b + 1) * D, :] = spread(flat[at:at + D // 8, :]).astype(F32)
        for i in range(F):
            for k in range(R):
                @pl.when(r == k)
                def _():
                    at = fwl + i * (FF // F) + k * fw
                    a4s[i * fw:(i + 1) * fw, :] = a4s[at:at + fw, :]
        z4_ref[...] = low(a4s[:fwl, :])
    for c in range(D // LANE):
        bt2_ref[:, c * LANE:(c + 1) * LANE] = tiled(cols(2, c))
        bt4_ref[:, c * LANE:(c + 1) * LANE] = tiled(cols(4, c))
    for c in range(3 * D // LANE):
        wide[:, c * LANE:(c + 1) * LANE] = cols(1, c)
    pad1[...] = jnp.zeros_like(pad1)
    for k in range(R):
        @pl.when(r == k)
        def _():
            for i in range(3 * hl):
                start = (i // hl) * D + (k * hl + i % hl) * HEAD_DIM
                pad1[:, i * LANE:i * LANE + HEAD_DIM] = wide[:, start:start + HEAD_DIM]
    bt1_ref[...] = tiled(pad1[...])
    for c in range(FF // LANE):
        wide[:, c * LANE:(c + 1) * LANE] = cols(3, c)
    for k in range(R):
        @pl.when(r == k)
        def _():
            for i in range(F):
                start = i * (FF // F) + k * fw
                pad1[:, i * fw:(i + 1) * fw] = wide[:, start:start + fw]
    bt3_ref[...] = tiled(pad1[:, :fwl])
    for c in range(6 * D // LANE):
        b0_ref[:, c * LANE:(c + 1) * LANE] = cols(0, c)
    u0 = low(tile_sum(mm(low(cs_ref[...]), z0_ref[...])))[0:1, :].astype(F32)
    u0c = jnp.broadcast_to(u0, (LANE, LANE)).T[:RANK, :]
    u0c_ref[...] = u0c
    over_fsdp(lambda i: mcopy(i, lax.rem(f + i, F)).wait_recv())
    total = mrecv[0]
    for l in range(1, F):
        total = total + mrecv[l]
    mods_ref[...] = total
    for c in range(6 * D // LANE):
        j, k = c // (D // LANE), c % (D // LANE)
        extra = 2.0 * jnp.sum(b0_ref[:, c * LANE:(c + 1) * LANE] * u0c, axis=0, keepdims=True)
        mods_ref[j:j + 1, k * LANE:(k + 1) * LANE] += extra
    for i in range(1, R):
        lcopy(i, lax.rem(r + i, R)).wait_recv()
        lcopy(i, r).wait_send()

    @pl.when(r < Q)
    def _():
        for i in range(1, R):
            acopy(i, r).wait_send()
        for owner in range(F):
            @pl.when(f == owner)
            def _():
                over_fsdp(lambda i: scopy(i, f, width[owner]).wait_send())

    over_fsdp(lambda i: icopy(i, f).wait_send())
    over_fsdp(lambda i: mcopy(i, f).wait_send())


def tail_kernel(R, lay, hl, dmm_ref, dma_ref, da1_ref, db1_ref, da2_ref, db2_ref, da3_ref, db3_ref, da4_ref, db4_ref,
                idx_ref, cs_ref, u0c_ref, b0_ref, z0_ref, wmod_ref, master_ref, m1_ref, m2_ref,
                dcs_ref, nm_ref, nm1_ref, nm2_ref, low_ref,
                sel, flat, wide, psend, precv, hs, orecv, gall, dsend, drecv, dall, csend, crecv,
                ds_sem, dr_sem, ps_sem, pr_sem, os_sem, or_sem, as_sem, ar_sem, gs_sem, gr_sem, cs_sem, cr_sem):
    F, Q, UQ, UR = lay.F, PARTS, lay.part, lay.rows
    r = lax.axis_index("rep")
    f = lax.axis_index("fsdp")
    rows = wmod_ref.shape[0]
    fw = FF // (F * R)
    fwl = F * fw
    early = lay.slot[2]
    ns = lay.slots - early
    full_barrier(R, r, F, f)

    def over_fsdp(step):
        def one(i, _):
            step(i)
            return 0

        lax.fori_loop(1, F, one, 0)

    dsend[...] = jnp.zeros_like(dsend)
    dsend[0:3, :] = dma_ref[0:3, :]
    dsend[3:6, :] = dmm_ref[0:3, :]

    def dcopy(i, who):
        return rep_copy(dsend, drecv.at[who], ds_sem.at[i], dr_sem.at[who], lax.rem(r + i, R))

    for i in range(1, R):
        dcopy(i, r).start()
    sel[...] = jnp.where(iota((D // 8, D), 1) // 8 == iota((D // 8, D), 0), 1.0, 0.0).astype(BF16)
    flat[...] = jnp.zeros_like(flat)
    keep = iota((LANE, D), 0) // RANK == iota((LANE, D), 1) % 8

    def a_rows(x):
        n = x.shape[1]
        return mm_t(sel[:n // 8, :n], low(jnp.where(keep[:, :n], jnp.concatenate([x] * 8, axis=0), 0.0)))

    def put_cols(j, x):
        nb = PAIRS[j][1] // LANE
        for c in range(nb):
            flat[pl.ds(lay.flat_row[2 * j + 1] + c, RANK, stride=nb), :] = x[:, c * LANE:(c + 1) * LANE]

    def place_hidden(ref):
        wide[...] = jnp.zeros_like(wide)
        for k in range(R):
            @pl.when(r == k)
            def _():
                for i in range(F):
                    start = i * (FF // F) + k * fw
                    wide[:, start:start + fw] = ref[:, i * fw:(i + 1) * fw]

    for j, ref in ((1, da1_ref), (2, da2_ref), (3, da3_ref)):
        flat[lay.flat_row[2 * j]:lay.flat_row[2 * j] + D // 8, :] = a_rows(ref[...])
    if fw % 8 == 0:
        y4 = a_rows(da4_ref[...])
        for k in range(R):
            @pl.when(r == k)
            def _():
                for i in range(F):
                    at = lay.flat_row[8] + (i * (FF // F) + k * fw) // 8
                    flat[at:at + fw // 8, :] = y4[i * fw // 8:(i + 1) * fw // 8, :]
    else:
        place_hidden(da4_ref)
        for b in range(FF // D):
            at = lay.flat_row[8] + b * D // 8
            flat[at:at + D // 8, :] = a_rows(wide[:, b * D:(b + 1) * D])
    put_cols(2, db2_ref)
    put_cols(4, db4_ref)
    wide[...] = jnp.zeros_like(wide)
    for k in range(R):
        @pl.when(r == k)
        def _():
            for i in range(3 * hl):
                start = (i // hl) * D + (k * hl + i % hl) * HEAD_DIM
                wide[:, start:start + HEAD_DIM] = db1_ref[:, i * LANE:i * LANE + HEAD_DIM]
    put_cols(1, wide)
    place_hidden(db3_ref)
    put_cols(3, wide)
    for q in range(Q):
        def pack(s, _):
            psend[q, s] = low(flat[pl.ds((s + early) * UR + q * UQ, UQ), :])
            return 0

        lax.fori_loop(0, ns, pack, 0)

    def pcopy(q, who):
        return rep_copy(psend.at[q], precv.at[who], ps_sem.at[q], pr_sem.at[who], q)

    for q in range(Q):
        @pl.when(r != q)
        def _():
            pcopy(q, r).start()
    for i in range(1, R):
        dcopy(i, lax.rem(r + i, R)).wait_recv()
    drecv[r] = dsend[...]
    total = drecv[0]
    for p in range(1, R):
        total = total + drecv[p]
    dall[f] = total

    def gcopy(i, who):
        return fsdp_copy(dall.at[f], dall.at[who], gs_sem.at[i], gr_sem.at[who], lax.rem(f + i, F))

    over_fsdp(lambda i: gcopy(i, f).start())
    du0 = jnp.zeros((RANK, 1), F32)
    u0c = u0c_ref[...]
    for j in range(6):
        row = total[j:j + 1, :]
        du0 = du0 + jnp.sum(b0_ref[:, j * D:(j + 1) * D] * row, axis=1, keepdims=True)
    du0 = 2.0 * du0
    nb = 6 * D // LANE
    for c in range(nb):
        j, k = c // (D // LANE), c % (D // LANE)
        flat[pl.ds(lay.flat_row[1] + c, RANK, stride=nb), :] = 2.0 * u0c * total[j:j + 1, k * LANE:(k + 1) * LANE]
    flat[0:D // 8, :] = a_rows(du0 * cs_ref[0:1, :])
    @pl.when(r < Q)
    def _():
        precv[r] = psend[jnp.minimum(r, Q - 1)]

        def pack(s, _):
            hs[s] = low(flat[pl.ds(s * UR + r * UQ, UQ), :])
            return 0

        lax.fori_loop(0, early, pack, 0)
        for p in range(R):
            @pl.when(r != p)
            def _():
                pcopy(r, p).wait_recv()

        def add(s, _):
            total = precv[0, s].astype(F32)
            for p in range(1, R):
                total = total + precv[p, s].astype(F32)
            hs[early + s] = low(total)
            return 0

        lax.fori_loop(0, ns, add, 0)

        def ocopy(owner, who):
            n = lay.hi[owner] - lay.lo[owner]
            return fsdp_copy(hs.at[pl.ds(lay.lo[owner], n)], orecv.at[who, pl.ds(0, n)], os_sem.at[owner], or_sem.at[who], owner)

        for owner in range(F):
            @pl.when(f != owner)
            def _():
                ocopy(owner, f).start()
        for owner in range(F):
            @pl.when(f == owner)
            def _():
                n = lay.hi[owner] - lay.lo[owner]
                orecv[owner, :n] = hs[lay.lo[owner]:lay.hi[owner]]
                for l in range(F):
                    if l != owner:
                        ocopy(owner, l).wait_recv()
        lo = lay.low_of(f)

        def gather_unit(u, _):
            j, a, s = lay.find(f * UNIT_COUNT + u)

            def each(l, total):
                hit = idx_ref[l, pl.ds(1 + j, 1), :][:, :LANE] == a.astype(F32)
                return total + jnp.where(hit, orecv[l, s - lo].astype(F32), 0.0)

            gall[r, u] = low(lax.fori_loop(0, F, each, jnp.zeros((UQ, LANE), F32)))
            return 0

        lax.fori_loop(0, UNIT_COUNT, gather_unit, 0)
        for owner in range(F):
            @pl.when(f != owner)
            def _():
                ocopy(owner, f).wait_send()

    def acopy(i, who):
        return rep_copy(gall.at[r], gall.at[who], as_sem.at[i], ar_sem.at[who], lax.rem(r + i, R))

    @pl.when(r < Q)
    def _():
        for i in range(1, R):
            acopy(i, r).start()
    over_fsdp(lambda i: gcopy(i, lax.rem(f + i, F)).wait_recv())
    dcs = jnp.zeros((2 * F, rows), F32)
    for j in range(6):
        x = jnp.concatenate([dall[l, j:j + 1, :] for l in range(F)], axis=0)
        hi = low(x)
        x = jnp.concatenate([hi, low(x - hi.astype(F32))], axis=0)
        dcs = dcs + mm_t(x, wmod_ref[:, j * D:(j + 1) * D])
    dcs = dcs[:F] + dcs[F:]
    for l in range(F):
        csend[l, 0:1, :rows] = dcs[l:l + 1, :]

    def ccopy(i, who):
        peer = lax.rem(f + i, F)
        return fsdp_copy(csend.at[peer], crecv.at[who], cs_sem.at[i], cr_sem.at[who], peer)

    over_fsdp(lambda i: ccopy(i, f).start())
    crecv[f] = csend[f]
    du0t = jnp.broadcast_to(jnp.concatenate([du0] * 8, axis=0), (LANE, LANE)).T[0:8, :]
    hi = low(du0t)
    extra = (mm_t(hi, z0_ref[...]) + mm_t(low(du0t - hi.astype(F32)), z0_ref[...]))[0:1, :]
    over_fsdp(lambda i: ccopy(i, lax.rem(f + i, F)).wait_recv())
    for l in range(F):
        dcs_ref[0:1, l * rows:(l + 1) * rows] = crecv[l, 0:1, :rows] + extra[:, l * rows:(l + 1) * rows]
    for q in range(Q):
        @pl.when(r != q)
        def _():
            acopy(lax.rem(q - r + R, R), q).wait_recv()

        def unpack(u, _):
            flat[pl.ds(u * UR + q * UQ, UQ), :] = gall[q, u].astype(F32)
            return 0

        lax.fori_loop(0, UNIT_COUNT, unpack, 0)
    corr = 1.0 - 0.5 ** STEP

    def adam(u, _):
        at = pl.ds(u * UR, UR)
        g = flat[at, :]
        p = master_ref[at, :]
        a = 0.5 * m1_ref[at, :] + 0.5 * g
        b = 0.5 * m2_ref[at, :] + 0.5 * g * g
        new = p - 0.01 * ((a / corr) / (jnp.sqrt(b / corr) + 1e-08) + 0.1 * p)
        nm1_ref[at, :] = a
        nm2_ref[at, :] = b
        nm_ref[at, :] = new
        low_ref[u] = low(new)
        return 0

    lax.fori_loop(0, UNIT_COUNT, adam, 0)
    for i in range(1, R):
        dcopy(i, r).wait_send()
    for q in range(Q):
        @pl.when(r != q)
        def _():
            pcopy(q, r).wait_send()
    over_fsdp(lambda i: gcopy(i, f).wait_send())
    over_fsdp(lambda i: ccopy(i, f).wait_send())

    @pl.when(r < Q)
    def _():
        for i in range(1, R):
            acopy(i, r).wait_send()


def shards(latents, condition, adapter_index, weight_mod, weight_qkv, weight_proj, weight_fc1, weight_fc2,
           master, moment1, moment2, cotangent):
    R = lax.axis_size("rep")
    F = lax.axis_size("fsdp")
    r = lax.axis_index("rep")
    f = lax.axis_index("fsdp")
    T = latents.shape[1]
    L = T * R
    hl = HEADS // R
    cw = hl * HEAD_DIM
    fw = FF // (F * R)
    rows = weight_qkv.shape[0]
    scale = HEAD_DIM ** -0.5

    def gather(x, axis_name, axis=0):
        return lax.all_gather(x, axis_name, axis=axis, tiled=True)

    def pick(x, axis):
        return lax.dynamic_index_in_dim(x, r, axis, keepdims=False)

    wqkv = gather(pick(weight_qkv.reshape(rows, 3, R, cw), 2).reshape(rows, 3 * cw), "fsdp")
    wproj = gather(weight_proj, "fsdp")
    w1 = gather(pick(weight_fc1.reshape(rows, F, R, fw), 2).reshape(rows, F * fw), "fsdp")
    w2 = gather(pick(weight_fc2.reshape(R, fw, D), 0), "fsdp")
    lay = Layout(F)
    UR, UQ, C, NS = lay.rows, lay.part, lay.most, lay.slots
    FW = F * fw
    W3 = 3 * hl * LANE
    cond = condition.astype(F32)
    sig = jax.nn.sigmoid(cond)
    cs = low(cond * sig).astype(F32)
    msg = jnp.pad(cs.reshape(F, 1, rows), ((0, 0), (0, 7), (0, 2 * LANE - rows)))
    picks = jnp.pad(adapter_index.astype(F32)[0], (1, 2)).reshape(1, 8, 1)
    msg = msg + picks
    part = jnp.minimum(r, PARTS - 1)
    units = lax.dynamic_index_in_dim(master.reshape(UNIT_COUNT, PARTS, UQ, LANE), part, 1, keepdims=False)
    cs8 = jnp.broadcast_to(cs, (8, D))
    (lat_all, idx, mods, u0c, b0, z0, z1, bt1, z2, bt2, z3, bt3, z4, bt4) = call(
        functools.partial(front_kernel, R, lay, hl), 4,
        [sds((L, D), BF16), sds((F, 8, 2 * LANE), F32), sds((8, D), F32), sds((RANK, LANE), F32), sds((RANK, 6 * D), F32),
         sds((D, LANE), BF16), sds((D, LANE), BF16), sds((LANE, W3), BF16), sds((D, LANE), BF16), sds((LANE, D), BF16),
         sds((D, LANE), BF16), sds((LANE, FW), BF16), sds((FW, LANE), BF16), sds((LANE, D), BF16)],
        [pltpu.VMEM((D, D // 8), BF16), pltpu.VMEM((F, C, UQ, LANE), BF16), pltpu.VMEM((F, C, UQ, LANE), BF16),
         pltpu.VMEM((R, NS, UQ, LANE), BF16), pltpu.VMEM((NS * UR, LANE), F32), pltpu.VMEM((F, 8, D), F32),
         pltpu.VMEM((F, 8, D), F32), pltpu.VMEM((RANK, FF), F32), pltpu.VMEM((RANK, max(W3, FW)), F32),
         pltpu.VMEM((FW // 8 if fw % 8 == 0 else FW + FF, LANE), F32)]
        + [dma(R)] * 2 + [dma(F)] * 6 + [dma(R)] * 2,
        latents[0], msg, weight_mod, units, cs8)
    h1, u1, qkv, lse, mixed, u2, ao, x1, h2a, douta = call(
        functools.partial(attn_fwd_kernel, R, hl, scale), 1,
        [sds((L, D), BF16), sds((L, LANE), BF16), sds((L, W3), BF16), sds((hl * 8, L), F32), sds((T, D), BF16),
         sds((T, LANE), BF16), sds((T, D), F32), sds((T, D), F32), sds((L, D), BF16), sds((L, D), BF16)],
        [pltpu.VMEM((D, W3), BF16), pltpu.VMEM((hl * LANE, L), BF16), pltpu.VMEM((hl, T, LANE), F32),
         pltpu.VMEM((L, cw), BF16), pltpu.VMEM((R, T, cw), BF16)] + [dma(R)] * 6,
        lat_all, cotangent[0], mods, wqkv, z1, bt1, wproj, z2, bt2)
    out, dx1, dmod_m, dA3, dB3, dA4, dB4 = call(
        functools.partial(mlp_kernel, R), 2,
        [sds((T, D), BF16), sds((T, D), F32), sds((8, D), F32), sds((RANK, D), F32), sds((RANK, FW), F32),
         sds((RANK, FW), F32), sds((RANK, D), F32)],
        [pltpu.VMEM((L, FW), BF16), pltpu.VMEM((L, FW), F32)] + [pltpu.VMEM((L, LANE), BF16)] * 4
        + [pltpu.VMEM((L, FW), BF16)]
        + [pltpu.VMEM((L, D), BF16), pltpu.VMEM((R, T, D), BF16), pltpu.VMEM((T, D), F32)] * 2 + [dma(R)] * 4,
        h2a, douta, mods, w1, z3, bt3, w2, z4, bt4, x1)
    lg, dmod_a, dA2, dB2, dA1, dB1 = call(
        functools.partial(attn_bwd_kernel, R, hl, scale), 3,
        [sds((T, D), F32), sds((8, D), F32), sds((RANK, D), F32), sds((RANK, D), F32), sds((RANK, D), F32),
         sds((RANK, W3), F32)],
        [pltpu.VMEM((D, W3), BF16), pltpu.VMEM((hl * LANE, L), BF16), pltpu.VMEM((R, T, cw), BF16),
         pltpu.VMEM((R, T, cw), BF16), pltpu.VMEM((hl, T, LANE), BF16), pltpu.VMEM((L, 2 * hl * LANE), F32),
         pltpu.VMEM((L, W3), BF16), pltpu.VMEM((L, LANE), BF16), pltpu.VMEM((L, D), BF16), pltpu.VMEM((R, T, D), BF16),
         pltpu.VMEM((T, D), F32)] + [dma(R)] * 4,
        dx1, ao, mods, wproj, z2, bt2, mixed, u2, qkv, lse, wqkv, z1, bt1, h1, u1, latents[0])
    SR = UNIT_COUNT * UR
    state = [x.reshape(SR, LANE) for x in (master, moment1, moment2)]
    d_cs, nm, nm1, nm2, nml = call(
        functools.partial(tail_kernel, R, lay, hl), 5,
        [sds((1, D), F32)] + [sds((SR, LANE), F32)] * 3 + [sds((UNIT_COUNT, UR, LANE), BF16)],
        [pltpu.VMEM((D // 8, D), BF16), pltpu.VMEM((NS * UR, LANE), F32), pltpu.VMEM((RANK, FF), F32),
         pltpu.VMEM((PARTS, NS - lay.slot[2], UQ, LANE), BF16), pltpu.VMEM((R, NS - lay.slot[2], UQ, LANE), BF16),
         pltpu.VMEM((NS, UQ, LANE), BF16), pltpu.VMEM((F, C, UQ, LANE), BF16), pltpu.VMEM((R, UNIT_COUNT, UQ, LANE), BF16),
         pltpu.VMEM((8, D), F32), pltpu.VMEM((R, 8, D), F32), pltpu.VMEM((F, 8, D), F32),
         pltpu.VMEM((F, 8, 2 * LANE), F32), pltpu.VMEM((F, 8, 2 * LANE), F32)]
        + [dma(R)] * 2 + [dma(PARTS), dma(R)] + [dma(F)] * 2 + [dma(R)] * 2 + [dma(F)] * 4,
        dmod_m, dmod_a, dA1, dB1, dA2, dB2, dA3, dB3, dA4, dB4, idx, cs8, u0c, b0, z0, weight_mod, *state)
    condition_grad = d_cs * (sig * (1.0 + cond * (1.0 - sig)))
    nm, nm1, nm2, nml = [x.reshape(-1) for x in (nm, nm1, nm2, nml)]
    return (out[None], lg[None], condition_grad, nm, nm1, nm2, nml)


def solution(mesh):
    tok = P("fsdp", "rep", None)
    row = P("fsdp", None)
    vec = P("fsdp")
    return jax.shard_map(shards, mesh=mesh,
                         in_specs=(tok, row, row, row, row, row, row, row, vec, vec, vec, tok),
                         out_specs=(tok, tok, row, vec, vec, vec, vec), check_vma=False)
```

```python
import functools

import jax
import jax.numpy as jnp
from jax import lax
from jax.experimental import pallas as pl
from jax.experimental.pallas import tpu as pltpu
from jax.sharding import PartitionSpec as P

D = 1152
HEAD_DIM = 72
HEADS = 16
FF = 4608
RANK = 16
ADAPT = 8
STEP = 3
NORM_EPS = 1e-06
F32 = jnp.float32
BF16 = jnp.bfloat16
PAIRS = ((D, 6 * D), (D, 3 * D), (D, D), (D, FF), (FF, D))


def dot(a, b, dims, **kw):
    return lax.dot_general(a, b, (dims, ((), ())), preferred_element_type=F32, **kw)


def mm(a, b):
    return dot(a, b, ((1,), (0,)))


def mm_t(a, b):
    return dot(a, b, ((1,), (1,)))


def tmm(a, b):
    return dot(a, b, ((0,), (0,)))


def low(v):
    return v.astype(BF16)


def layer_norm(v):
    centred = v - jnp.mean(v, axis=-1, keepdims=True)
    inv = lax.rsqrt(jnp.mean(centred * centred, axis=-1, keepdims=True) + NORM_EPS)
    return centred * inv, inv


def layer_norm_back(g, normed, inv):
    m1 = jnp.mean(g, axis=-1, keepdims=True)
    m2 = jnp.mean(g * normed, axis=-1, keepdims=True)
    return inv * (g - m1 - normed * m2)


LANE = 128
GELU_C = 0.7978845608028654
GELU_A = 0.044715


def tile_sum(v):
    shift = LANE // 2
    while shift >= RANK:
        v = v + pltpu.roll(v, shift, 1)
        shift //= 2
    return v


def rep_copy(src, dst, send, recv, peer):
    return pltpu.make_async_remote_copy(src_ref=src, dst_ref=dst, send_sem=send, recv_sem=recv,
                                        device_id={"rep": peer}, device_id_type=pl.DeviceIdType.MESH)


def rep_barrier(R, r):
    sem = pltpu.get_barrier_semaphore()
    for i in range(1, R):
        pl.semaphore_signal(sem, inc=1, device_id={"rep": lax.rem(r + i, R)}, device_id_type=pl.DeviceIdType.MESH)
    pl.semaphore_wait(sem, R - 1)


def block(i, n):
    return pl.ds(pl.multiple_of(i * n, n), n)


def whole(ref):
    n = ref.shape[0] * ref.shape[1]
    if ref.shape[1] % 16 == 0:
        return ref[...].reshape(n, ref.shape[2])
    return low(jnp.concatenate([ref[i].astype(F32) for i in range(ref.shape[0])], axis=0))


PARTS = 4
UNIT_COUNT = 23
TABLES = (1, 6, 1, 3, 1, 1, 1, 4, 4, 1)


class Layout:
    def __init__(self, F):
        self.F = F
        self.n = [t * F // 8 for t in TABLES]
        self.first = [ADAPT * sum(self.n[:j]) for j in range(11)]
        self.slot = [sum(self.n[:j]) for j in range(11)]
        self.slots = self.slot[10]
        self.rows = D // F
        self.part = self.rows // PARTS
        self.lo, self.hi = [], []
        for f in range(F):
            held = [self.slot_of(g) for g in range(UNIT_COUNT * f, UNIT_COUNT * (f + 1))]
            self.lo.append(min(held))
            self.hi.append(max(held) + 1)
        self.most = max(h - l for h, l in zip(self.hi, self.lo))
        self.flat_row = [s * self.rows for s in self.slot]

    def slot_of(self, g):
        j = max(j for j in range(10) if self.first[j] <= g)
        return self.slot[j] + (g - self.first[j]) % self.n[j]

    def low_of(self, f):
        lo = self.lo[0] + 0 * f
        for i in range(1, self.F):
            lo = jnp.where(f == i, self.lo[i], lo)
        return lo

    def find(self, g):
        j, a, s = 0 * g, g // self.n[0], g % self.n[0]
        for t in range(1, 10):
            here = g >= self.first[t]
            rest = g - self.first[t]
            j = jnp.where(here, t // 2, j)
            a = jnp.where(here, rest // self.n[t], a)
            s = jnp.where(here, self.slot[t] + rest % self.n[t], s)
        return j, a, s


def fsdp_copy(src, dst, send, recv, peer):
    return pltpu.make_async_remote_copy(src_ref=src, dst_ref=dst, send_sem=send, recv_sem=recv,
                                        device_id={"fsdp": peer}, device_id_type=pl.DeviceIdType.MESH)


def full_barrier(R, r, F, f):
    sem = pltpu.get_barrier_semaphore()
    for i in range(1, R):
        pl.semaphore_signal(sem, inc=1, device_id={"rep": lax.rem(r + i, R)}, device_id_type=pl.DeviceIdType.MESH)
    for i in range(1, F):
        pl.semaphore_signal(sem, inc=1, device_id={"fsdp": lax.rem(f + i, F)}, device_id_type=pl.DeviceIdType.MESH)
    pl.semaphore_wait(sem, R + F - 2)


def iota(shape, axis):
    return lax.broadcasted_iota(jnp.int32, shape, axis)


def slice_kernel(R, F, wqkv_ref, w1_ref, w2_ref, wqs_ref, w1s_ref, w2s_ref):
    r = lax.axis_index("rep")
    cw = D // R
    fw = FF // (F * R)
    for k in range(R):
        @pl.when(r == k)
        def _():
            for j in range(3):
                wqs_ref[:, j * cw:(j + 1) * cw] = wqkv_ref[:, j * D + k * cw:j * D + (k + 1) * cw]
            for i in range(F):
                at = i * (FF // F) + k * fw
                w1s_ref[:, i * fw:(i + 1) * fw] = w1_ref[:, at:at + fw]
            if w2_ref is not None:
                w2s_ref[...] = w2_ref[k * fw:(k + 1) * fw, :]


def step_kernel(R, lay, hl, scale, lat_ref, dout_ref, cond_ref, pick_ref, wmod_ref, master_ref, wqs_ref, wproj_ref, w1s_ref, w2s_ref,
                idx_ref, u0c_ref, b0_ref, z0_ref, out_ref, lg_ref, dmod_ref,
                da3_ref, db3_ref, da4_ref, db4_ref, da2_ref, db2_ref, da1_ref, db1_ref,
                mods_v, z1_v, bt1_v, z2_v, bt2_v, z3_v, bt3_v, z4_v, bt4_v, wq, wp, w1, w2,
                h1_v, u1_v, qkv_v, lse_v, mixed_v, u2_v, ao_v, douta_v,
                lata, msg, vt, osc, xsend, xrecv, rbuf, parts, nrecv,
                h2a, precv, pown, gsend, grecv, gown, msend,
                load_sem, ls_sem, lr_sem, is_sem, ir_sem, ss_sem, sr_sem, ns_sem, nr_sem, as_sem, ar_sem,
                q_sem, o_sem, a_sem, b_sem, ds_sem, dr_sem, xs_sem, xr_sem,
                hs_sem, hr_sem, ps_sem, pr_sem, gs_sem, gr_sem, ms_sem, mr_sem, ts_sem, tr_sem):
    F, Q, UQ, UR = lay.F, PARTS, lay.part, lay.rows
    r = lax.axis_index("rep")
    f = lax.axis_index("fsdp")
    T = lat_ref.shape[0]
    rows = wqs_ref.shape[0]
    fw = FF // (F * R)
    L = T * R
    cw = hl * HEAD_DIM
    full_barrier(R, r, F, f)
    P2 = F // 2
    chip, core = f // 2, lax.rem(f, 2)
    mate = chip * 2 + 1 - core
    cond = cond_ref[...].astype(F32)
    cs = low(cond / (1.0 + jnp.exp(-cond))).astype(F32)
    msg[...] = jnp.zeros_like(msg)
    for i in range(F):
        msg[i, 0:1, :rows] = cs[:, i * rows:(i + 1) * rows]
        for j in range(5):
            msg[i, 1 + j:2 + j, :] = jnp.full((1, 2 * LANE), pick_ref[0, j], jnp.int32).astype(F32)

    def icopy(i, who):
        peer = lax.rem(f + i, F)
        return fsdp_copy(msg.at[peer], idx_ref.at[who], is_sem.at[i], ir_sem.at[who], peer)

    def lcopy(i, who):
        return rep_copy(lat_ref, lata.at[block(who, T)], ls_sem.at[i], lr_sem.at[who], lax.rem(r + i, R))

    def over_fsdp(step):
        def one(i, _):
            step(i)
            return 0

        lax.fori_loop(1, F, one, 0)

    width = [h - l for h, l in zip(lay.hi, lay.lo)]
    def bcopy(src, buf, sems, b):
        return fsdp_copy(src, buf.at[b], sems.at[4, b], sems.at[5, b], mate)

    def up(src, buf, sems, b):
        return fsdp_copy(src, buf.at[b], sems.at[0, b], sems.at[1, b], lax.rem(f + 2, F))

    def down(src, buf, sems, b):
        return fsdp_copy(src, buf.at[b], sems.at[2, b], sems.at[3, b], lax.rem(f - 2 + F, F))

    def relay_start(src, buf, sems):
        @pl.when(chip < P2 - 1)
        def _():
            up(src, buf, sems, f).start()

        @pl.when(chip > 0)
        def _():
            down(src, buf, sems, f).start()
        bcopy(src, buf, sems, f).start()
        buf[f] = src[...]

    def relay(src, buf, sems, t):
        lo_b, hi_b = f - 2 * t, f + 2 * t

        @pl.when(chip >= t)
        def _():
            up(src, buf, sems, lo_b).wait_recv()

            @pl.when(chip < P2 - 1)
            def _():
                up(buf.at[lo_b], buf, sems, lo_b).start()
            bcopy(buf.at[lo_b], buf, sems, lo_b).start()

        @pl.when(chip + t < P2)
        def _():
            down(src, buf, sems, hi_b).wait_recv()

            @pl.when(chip > 0)
            def _():
                down(buf.at[hi_b], buf, sems, hi_b).start()
            bcopy(buf.at[hi_b], buf, sems, hi_b).start()

    def relay_rest(src, buf, sems, t0):
        def one(t, _):
            relay(src, buf, sems, t)
            return 0

        if t0 < P2:
            lax.fori_loop(t0, P2, one, 0)

    def relay_wait(src, buf, sems):
        def one(p, _):
            bcopy(src, buf, sems, 2 * p + 1 - core).wait_recv()
            return 0

        lax.fori_loop(0, P2, one, 0)

    def relay_close(src, buf, sems):
        def one(p, _):
            b = 2 * p + core

            @pl.when((p <= chip) & (chip < P2 - 1))
            def _():
                up(src, buf, sems, b).wait_send()

            @pl.when((p >= chip) & (chip > 0))
            def _():
                down(src, buf, sems, b).wait_send()
            bcopy(src, buf, sems, b).wait_send()
            return 0

        lax.fori_loop(0, P2, one, 0)

    q_way = (wqs_ref, wq, q_sem)
    o_way = (wproj_ref, wp, o_sem)
    a_way = (w1s_ref, w1, a_sem)
    b_way = (w2s_ref, w2, b_sem)
    def acopy(i, who):
        return rep_copy(parts.at[r], parts.at[who], as_sem.at[i], ar_sem.at[who], lax.rem(r + i, R))

    def dcopy(i, who):
        return rep_copy(dout_ref, douta_v.at[block(who, T)], ds_sem.at[i], dr_sem.at[who], lax.rem(r + i, R))

    over_fsdp(lambda i: icopy(i, f).start())
    for i in range(1, R):
        lcopy(i, r).start()
    def front(sel, flat, wide, pad1, a4s, wmod, master, sbuf, nsend):
        def scopy(i, who, n):
            peer = lax.rem(f + i, F)
            return fsdp_copy(sbuf.at[peer, pl.ds(0, n)], rbuf.at[who, pl.ds(0, n)], ss_sem.at[i], sr_sem.at[who], peer)

        def ncopy(i, who):
            peer = lax.rem(f + i, F)
            return fsdp_copy(nsend.at[peer], nrecv.at[who], ns_sem.at[i], nr_sem.at[who], peer)

        pltpu.make_async_copy(master_ref, master, load_sem.at[0]).start()
        pltpu.make_async_copy(wmod_ref, wmod, load_sem.at[1]).start()
        idx_ref[f] = msg[f]
        lata[block(r, T), :] = lat_ref[...]
        sel[...] = jnp.where(iota((D, D // 8), 0) // 8 == iota((D, D // 8), 1), 1.0, 0.0).astype(BF16)
        sbuf[...] = jnp.zeros_like(sbuf)
        over_fsdp(lambda i: icopy(i, lax.rem(f + i, F)).wait_recv())
        lo = lay.low_of(f)
        part = jnp.minimum(r, Q - 1)

        pltpu.make_async_copy(master_ref, master, load_sem.at[0]).wait()

        def choose(u, _):
            j, a, s = lay.find(f * UNIT_COUNT + u)
            unit = master[pl.ds(u * UR + part * UQ, UQ), :]

            def each(l, _):
                hit = idx_ref[l, pl.ds(1 + j, 1), :][:, :LANE] == a.astype(F32)
                sbuf[l, s - lo] = low(jnp.where(hit, unit, sbuf[l, s - lo].astype(F32)))
                return 0

            return lax.fori_loop(0, F, each, 0)

        lax.fori_loop(0, UNIT_COUNT, choose, 0)

        for owner in range(F):
            @pl.when((f == owner) & (r < Q))
            def _():
                over_fsdp(lambda i: scopy(i, f, width[owner]).start())
        rbuf[f] = sbuf[f]
        chosen = low(jnp.concatenate([idx_ref[l, 0:1, :rows] for l in range(F)], axis=0))
        pltpu.make_async_copy(wmod_ref, wmod, load_sem.at[1]).wait()
        for j in range(6):
            piece = mm(chosen, wmod[:, j * D:(j + 1) * D])
            for l in range(F):
                nsend[l, j:j + 1, :] = piece[l:l + 1, :]

        over_fsdp(lambda i: ncopy(i, f).start())
        nrecv[f] = nsend[f]
        relay_start(*q_way)
        relay_start(*o_way)

        @pl.when(r < Q)
        def _():
            for owner in range(F):
                @pl.when(f != owner)
                def _():
                    scopy(lax.rem(owner - f + F, F), owner, width[owner]).wait_recv()
            for s in range(lay.slots):
                held = [o for o in range(F) if lay.lo[o] <= s < lay.hi[o]]
                total = rbuf[held[0], s - lay.lo[held[0]]].astype(F32)
                for o in held[1:]:
                    total = total + rbuf[o, s - lay.lo[o]].astype(F32)
                parts[r, s] = low(total)
            for i in range(1, R):
                acopy(i, r).start()

        for i in range(1, R):
            dcopy(i, r).start()
        douta_v[block(r, T), :] = dout_ref[...]

        relay(*q_way, 1)

        def arrived(q):
            @pl.when(r != q)
            def _():
                acopy(lax.rem(q - r + R, R), q).wait_recv()

        for q in range(Q):
            arrived(q)

            def unpack(s, _):
                flat[pl.ds(s * UR + q * UQ, UQ), :] = parts[q, s].astype(F32)
                return 0

            lax.fori_loop(0, lay.slots, unpack, 0)

        if P2 > 2:
            relay(*q_way, 2)
        keep = iota((D, LANE), 1) // RANK == iota((D, LANE), 0) % 8

        def spread(x):
            n = x.shape[0]
            return low(jnp.where(keep[:8 * n], mm(sel[:8 * n, :n], low(x)), 0.0))

        def cols(j, c):
            nb = PAIRS[j][1] // LANE
            return flat[pl.ds(lay.flat_row[2 * j + 1] + c, RANK, stride=nb), :]

        def tiled(x):
            return jnp.concatenate([low(x)] * 8, axis=0)

        def a_rows(j):
            return flat[lay.flat_row[2 * j]:lay.flat_row[2 * j] + D // 8, :]

        z0_ref[...] = spread(a_rows(0))
        z1_v[...] = spread(a_rows(1))
        z2_v[...] = spread(a_rows(2))
        z3_v[...] = spread(a_rows(3))
        fwl = F * fw
        if fw % 8 == 0:
            for i in range(F):
                for k in range(R):
                    @pl.when(r == k)
                    def _():
                        at = lay.flat_row[8] + (i * (FF // F) + k * fw) // 8
                        a4s[i * fw // 8:(i + 1) * fw // 8, :] = flat[at:at + fw // 8, :]
            z4_v[...] = spread(a4s[...])
        else:
            for b in range(FF // D):
                at = lay.flat_row[8] + b * D // 8
                a4s[fwl + b * D:fwl + (b + 1) * D, :] = spread(flat[at:at + D // 8, :]).astype(F32)
            for i in range(F):
                for k in range(R):
                    @pl.when(r == k)
                    def _():
                        at = fwl + i * (FF // F) + k * fw
                        a4s[i * fw:(i + 1) * fw, :] = a4s[at:at + fw, :]
            z4_v[...] = low(a4s[:fwl, :])
        for c in range(D // LANE):
            bt2_v[:, c * LANE:(c + 1) * LANE] = tiled(cols(2, c))
            bt4_v[:, c * LANE:(c + 1) * LANE] = tiled(cols(4, c))
        for c in range(3 * D // LANE):
            wide[:, c * LANE:(c + 1) * LANE] = cols(1, c)
        for k in range(R):
            @pl.when(r == k)
            def _():
                for j in range(3):
                    pad1[:, j * cw:(j + 1) * cw] = wide[:, j * D + k * cw:j * D + (k + 1) * cw]
        bt1_v[...] = tiled(pad1[:, :3 * cw])
        for c in range(FF // LANE):
            wide[:, c * LANE:(c + 1) * LANE] = cols(3, c)
        for k in range(R):
            @pl.when(r == k)
            def _():
                for i in range(F):
                    start = i * (FF // F) + k * fw
                    pad1[:, i * fw:(i + 1) * fw] = wide[:, start:start + fw]
        bt3_v[...] = tiled(pad1[:, :fwl])
        for c in range(6 * D // LANE):
            b0_ref[:, c * LANE:(c + 1) * LANE] = cols(0, c)
        u0 = low(tile_sum(mm(low(jnp.broadcast_to(cs, (8, D))), z0_ref[...])))[0:1, :].astype(F32)
        u0c = jnp.broadcast_to(u0, (LANE, LANE)).T[:RANK, :]
        u0c_ref[...] = u0c
        over_fsdp(lambda i: ncopy(i, lax.rem(f + i, F)).wait_recv())
        total = nrecv[0]
        for l in range(1, F):
            total = total + nrecv[l]
        mods_v[...] = total
        for c in range(6 * D // LANE):
            j, k = c // (D // LANE), c % (D // LANE)
            extra = 2.0 * jnp.sum(b0_ref[:, c * LANE:(c + 1) * LANE] * u0c, axis=0, keepdims=True)
            mods_v[j:j + 1, k * LANE:(k + 1) * LANE] += extra
        over_fsdp(lambda i: ncopy(i, f).wait_send())
        for owner in range(F):
            @pl.when((f == owner) & (r < Q))
            def _():
                over_fsdp(lambda i: scopy(i, f, width[owner]).wait_send())

    pl.run_scoped(front, pltpu.VMEM((D, D // 8), BF16), pltpu.VMEM((lay.slots * UR, LANE), F32), pltpu.VMEM((RANK, FF), F32),
                  pltpu.VMEM((RANK, max(3 * cw, F * fw)), F32),
                  pltpu.VMEM((F * fw // 8 if fw % 8 == 0 else F * fw + FF, LANE), F32),
                  pltpu.VMEM(wmod_ref.shape, BF16), pltpu.VMEM(master_ref.shape, F32),
                  pltpu.VMEM(rbuf.shape, BF16), pltpu.VMEM(nrecv.shape, F32))
    shift_a, scale_a, gate_a = mods_v[0:1, :], mods_v[1:2, :], mods_v[2:3, :]
    shift_m, scale_m = mods_v[3:4, :], mods_v[4:5, :]

    relay_rest(*q_way, 3)
    relay_start(*a_way)
    relay_start(*b_way)
    relay_wait(*q_way)
    qkv_v[...] = jnp.zeros_like(qkv_v)

    def first(c, _):
        p = lax.rem(r - c + R, R)
        rows = block(p, T)

        @pl.when(c > 0)
        def _():
            lcopy(c, p).wait_recv()
        n, _ = layer_norm(lata[rows, :].astype(F32))
        h1 = low(n * (1.0 + scale_a) + shift_a)
        h1_v[rows, :] = h1
        u1 = low(tile_sum(mm(h1, z1_v[...])))
        u1_v[rows, :] = u1
        u1 = u1 * BF16(0.25)
        x = low(mm(h1, whole(wq)) + mm(u1, bt1_v[...]))
        for i in range(3 * hl):
            qkv_v[rows, i * LANE:i * LANE + HEAD_DIM] = x[:, i * HEAD_DIM:(i + 1) * HEAD_DIM]
        return 0

    lax.fori_loop(0, R, first, 0)

    relay(*o_way, 1)

    def transpose_v(h, _):
        vt[block(h, LANE), :] = qkv_v[:, block(2 * hl + h, LANE)].T
        return 0

    lax.fori_loop(0, hl, transpose_v, 0)

    def xcopy(i, who):
        peer = lax.rem(r + i, R)
        return rep_copy(xsend.at[block(peer, T)], xrecv.at[who], xs_sem.at[i], xr_sem.at[who], peer)

    def attend(i, _):
        peer = lax.rem(r + 1 + i, R)
        rows = block(peer, T)

        def head(h, _):
            s = mm_t(qkv_v[:, block(hl + h, LANE)], qkv_v[rows, block(h, LANE)])
            top = jnp.max(s, axis=0, keepdims=True)
            e = jnp.exp((s - top) * scale)
            total = jnp.sum(e, axis=0, keepdims=True)
            lse_v[block(h, 8), rows] = jnp.broadcast_to(top * scale + jnp.log(total), (8, T))
            o = mm(vt[block(h, LANE), :], low(e * (1.0 / total)))
            osc[h] = o.T
            return 0

        lax.fori_loop(0, hl, head, 0)
        for h in range(hl):
            xsend[rows, h * HEAD_DIM:(h + 1) * HEAD_DIM] = low(osc[h][:, :HEAD_DIM])

        @pl.when(i < R - 1)
        def _():
            xcopy(i + 1, r).start()

        @pl.when((i == R // 2) & (P2 > 2))
        def _():
            relay(*o_way, 2)
        return 0

    lax.fori_loop(0, R, attend, 0)
    xrecv[r] = xsend[block(r, T), :]
    relay_rest(*o_way, 3)
    for i in range(1, R):
        xcopy(i, lax.rem(r + i, R)).wait_recv()
    for p in range(R):
        mixed_v[:, p * cw:(p + 1) * cw] = xrecv[p]
    mixed = mixed_v[...]
    u2 = low(tile_sum(mm(mixed, z2_v[...])))
    u2_v[...] = u2
    relay(*a_way, 1)
    relay_wait(*o_way)
    ao = mm(mixed, whole(wp)) + mm(u2 * BF16(0.25), bt2_v[...])
    ao_v[...] = ao
    x1 = lat_ref[...].astype(F32) + gate_a * ao
    n, _ = layer_norm(x1)
    h2a[block(r, T), :] = low(n * (1.0 + scale_m) + shift_m)
    def x1_of():
        return lat_ref[...].astype(F32) + mods_v[2:3, :] * ao_v[...]

    scale_m, gate_m = mods_v[4:5, :], mods_v[5:6, :]

    def pcopy(i, who):
        peer = lax.rem(r + i, R)
        return rep_copy(lata.at[block(peer, T)], precv.at[i - 1], ps_sem.at[i], pr_sem.at[who], peer)

    def gcopy(i, who):
        peer = lax.rem(r + i, R)
        return rep_copy(gsend.at[block(peer, T)], grecv.at[i - 1], gs_sem.at[i], gr_sem.at[who], peer)

    def hcopy(i, who):
        return rep_copy(h2a.at[block(r, T)], h2a.at[block(who, T)], hs_sem.at[i], hr_sem.at[who], lax.rem(r + i, R))

    for i in range(1, R):
        hcopy(i, r).start()
    relay_rest(*a_way, 2)
    relay_rest(*b_way, 1)
    relay_wait(*a_way)
    relay_wait(*b_way)

    def back(act, gp, u3s, u4s, du3s, dqs, mpad):
        def transpose_k(h, _):
            vt[block(h, LANE), :] = qkv_v[:, block(hl + h, LANE)].T
            return 0

        lax.fori_loop(0, hl, transpose_k, 0)

        def forward(i, _):
            peer = lax.rem(r - i + R, R)
            rows = block(peer, T)

            @pl.when(i > 0)
            def _():
                hcopy(i, peer).wait_recv()
            h2 = h2a[rows, :]
            u3 = low(tile_sum(mm(h2, z3_v[...])))
            u3s[rows, :] = u3
            x = mm(h2, whole(w1)) + mm(u3 * BF16(0.25), bt3_v[...])
            x2 = x * x
            t = jnp.tanh(GELU_C * (x + GELU_A * x * x2))
            a = low(0.5 * x * (1.0 + t))
            act[rows, :] = a
            gp[rows, :] = 0.5 * (1.0 + t) + 0.5 * x * (1.0 - t * t) * (GELU_C * (1.0 + 3.0 * GELU_A * x2))
            u4 = low(tile_sum(mm(a, z4_v[...])))
            u4s[rows, :] = u4
            part = mm(a, whole(w2)) + mm(u4 * BF16(0.25), bt4_v[...])
            lata[rows, :] = low(part)

            @pl.when(i == 0)
            def _():
                pown[...] = part
            return 0

        lax.fori_loop(0, R, forward, 0)
        da4_ref[...] = jnp.zeros_like(da4_ref)
        dmod_ref[...] = jnp.zeros_like(dmod_ref)

        def backward(i, _):
            peer = lax.rem(r + 1 + i, R)
            rows = block(peer, T)
            dm = low(douta_v[rows, :].astype(F32) * gate_m)
            douta_v[rows, :] = dm
            du4 = low(2.0 * mm_t(dm, bt4_v[...]))
            d_act = mm_t(dm, whole(w2)) + mm_t(du4, z4_v[...])
            dp = low(d_act * gp[rows, :])
            da4_ref[...] += tmm(du4, act[rows, :])[:RANK]
            act[rows, :] = dp
            du3 = low(2.0 * mm_t(dp, bt3_v[...]))
            du3s[rows, :] = du3
            part = mm_t(dp, whole(w1)) + mm_t(du3, z3_v[...])
            gsend[rows, :] = low(part)
            gown[...] = part

            @pl.when(i < R - 1)
            def _():
                gcopy(i + 1, r).start()
            return 0

        for i in range(1, R):
            dcopy(i, lax.rem(r + i, R)).wait_recv()
        lax.fori_loop(0, R, backward, 0)
        da3_ref[...] = tmm(du3s[...], h2a[...])[:RANK]
        n2, inv2 = layer_norm(x1_of())
        dh2 = gown[...]
        for i in range(1, R):
            p = lax.rem(r - i + R, R)
            gcopy(i, p).wait_recv()
            dh2 = dh2 + grecv[i - 1].astype(F32)
        dmod_ref[3:4, :] = jnp.sum(dh2, axis=0, keepdims=True)
        dmod_ref[4:5, :] = jnp.sum(dh2 * n2, axis=0, keepdims=True)
        dx1 = dout_ref[...].astype(F32) + layer_norm_back(dh2 * (1.0 + scale_m), n2, inv2)
        lg_ref[...] = dx1
        scale_a, gate_a = mods_v[1:2, :], mods_v[2:3, :]
        dmod_ref[2:3, :] = jnp.sum(dx1 * ao_v[...], axis=0, keepdims=True)
        da = low(dx1 * gate_a)
        du2 = low(2.0 * mm_t(da, bt2_v[...]))
        dm = low(mm_t(da, whole(wp)) + mm_t(du2, z2_v[...]))
        for p in range(R):
            msend[p] = dm[:, p * cw:(p + 1) * cw]

        def mcopy(i, who):
            peer = lax.rem(r + i, R)
            return rep_copy(msend.at[peer], xrecv.at[who], ms_sem.at[i], mr_sem.at[who], peer)

        for i in range(1, R):
            mcopy(i, r).start()
        xrecv[r] = msend[r]
        db2_ref[...] = 2.0 * tmm(u2_v[...], da)[:RANK]
        da2_ref[...] = tmm(du2, mixed_v[...])[:RANK]
        for i in range(1, R):
            pcopy(i, r).start()
        db4_ref[...] = 2.0 * tmm(u4s[...], douta_v[...])[:RANK]
        db3_ref[...] = 2.0 * tmm(u3s[...], act[...])[:RANK]
        dkv, dqkv = gp, act
        dkv[...] = jnp.zeros_like(dkv)
        mpad[...] = jnp.zeros_like(mpad)

        def attend(i, _):
            p = lax.rem(r + i, R)

            @pl.when(i > 0)
            def _():
                mcopy(i, p).wait_recv()
            for h in range(hl):
                mpad[h, :, :HEAD_DIM] = xrecv[p][:, h * HEAD_DIM:(h + 1) * HEAD_DIM]
            rows = block(p, T)

            def head(h, _):
                q = qkv_v[rows, block(h, LANE)]
                g = mpad[h]
                s = mm_t(qkv_v[:, block(hl + h, LANE)], q)
                lse = lse_v[block(h, 8), rows][0:1, :]
                probs = jnp.exp(s * scale - lse)
                dkv[:, block(hl + h, LANE)] += mm(low(probs), g)
                dp = mm_t(qkv_v[:, block(2 * hl + h, LANE)], g)
                centre = jnp.sum(probs * dp, axis=0, keepdims=True)
                ds = low(probs * (dp - centre))
                dkv[:, block(h, LANE)] += mm(ds, q)
                dq = mm(vt[block(h, LANE), :], ds)
                dqs[rows, block(h, LANE)] = low(dq.T * scale)
                return 0

            lax.fori_loop(0, hl, head, 0)
            return 0

        lax.fori_loop(0, R, attend, 0)

        def tcopy(i, who):
            peer = lax.rem(r + i, R)
            return rep_copy(gsend.at[block(peer, T)], grecv.at[i - 1], ts_sem.at[i], tr_sem.at[who], peer)

        for i in range(1, R):
            gcopy(i, r).wait_send()

        def backward(i, _):
            peer = lax.rem(r + 1 + i, R)
            rows = block(peer, T)
            for h in range(hl):
                dqkv[rows, h * HEAD_DIM:(h + 1) * HEAD_DIM] = dqs[rows, h * LANE:h * LANE + HEAD_DIM]
                at = (hl + h) * HEAD_DIM
                dqkv[rows, at:at + HEAD_DIM] = low(dkv[rows, h * LANE:h * LANE + HEAD_DIM] * scale)
                at = (2 * hl + h) * HEAD_DIM
                dqkv[rows, at:at + HEAD_DIM] = low(dkv[rows, (hl + h) * LANE:(hl + h) * LANE + HEAD_DIM])
            g = dqkv[rows, :3 * cw]
            du1 = low(2.0 * mm_t(g, bt1_v[...]))
            du3s[rows, :] = du1
            part = mm_t(g, whole(wq)) + mm_t(du1, z1_v[...])
            gsend[rows, :] = low(part)
            gown[...] = part

            @pl.when(i < R - 1)
            def _():
                tcopy(i + 1, r).start()
            return 0

        lax.fori_loop(0, R, backward, 0)
        da1_ref[...] = tmm(du3s[...], h1_v[...])[:RANK]
        db1_ref[...] = 2.0 * tmm(u1_v[...], dqkv[:, :3 * cw])[:RANK]
        mlp = pown[...]
        for i in range(1, R):
            p = lax.rem(r - i + R, R)
            pcopy(i, p).wait_recv()
            mlp = mlp + precv[i - 1].astype(F32)
        out_ref[...] = low(x1_of() + gate_m * mlp)
        dmod_ref[5:6, :] = jnp.sum(dout_ref[...].astype(F32) * mlp, axis=0, keepdims=True)
        n1, inv1 = layer_norm(lat_ref[...].astype(F32))
        dh1 = gown[...]
        for i in range(1, R):
            p = lax.rem(r - i + R, R)
            tcopy(i, p).wait_recv()
            dh1 = dh1 + grecv[i - 1].astype(F32)
        dmod_ref[0:1, :] = jnp.sum(dh1, axis=0, keepdims=True)
        dmod_ref[1:2, :] = jnp.sum(dh1 * n1, axis=0, keepdims=True)
        lg_ref[...] = lg_ref[...] + layer_norm_back(dh1 * (1.0 + scale_a), n1, inv1)
        for i in range(1, R):
            hcopy(i, r).wait_send()
            pcopy(i, r).wait_send()
            mcopy(i, r).wait_send()
            tcopy(i, r).wait_send()

    pl.run_scoped(back, pltpu.VMEM((L, max(F * fw, 3 * cw)), BF16), pltpu.VMEM((L, max(F * fw, 2 * hl * LANE)), F32),
                  pltpu.VMEM((L, LANE), BF16), pltpu.VMEM((L, LANE), BF16), pltpu.VMEM((L, LANE), BF16),
                  pltpu.VMEM((L, hl * LANE), BF16), pltpu.VMEM((hl, T, LANE), BF16))
    for i in range(1, R):
        dcopy(i, r).wait_send()
        xcopy(i, r).wait_send()
    for way in (q_way, o_way, a_way, b_way):
        relay_close(*way)
    for i in range(1, R):
        lcopy(i, r).wait_send()

    @pl.when(r < Q)
    def _():
        for i in range(1, R):
            acopy(i, r).wait_send()

    over_fsdp(lambda i: icopy(i, f).wait_send())


def tail_kernel(R, lay, hl, dmod_ref, da1_ref, db1_ref, da2_ref, db2_ref, da3_ref, db3_ref, da4_ref, db4_ref,
                idx_ref, cond_ref, u0c_ref, b0_ref, z0_ref, wmod_ref,
                dcs_ref, grad_ref,
                sel, flat, wide, psend, precv, hs, orecv, gall, drecv, dall, csend, crecv,
                ds_sem, dr_sem, ps_sem, pr_sem, os_sem, or_sem, as_sem, ar_sem, gs_sem, gr_sem, cs_sem, cr_sem):
    F, Q, UQ, UR = lay.F, PARTS, lay.part, lay.rows
    r = lax.axis_index("rep")
    f = lax.axis_index("fsdp")
    rows = wmod_ref.shape[0]
    fw = FF // (F * R)
    fwl = F * fw
    cw = hl * HEAD_DIM
    cond = cond_ref[...].astype(F32)
    sig = 1.0 / (1.0 + jnp.exp(-cond))
    slope = sig * (1.0 + cond * (1.0 - sig))
    early = lay.slot[2]
    ns = lay.slots - early
    full_barrier(R, r, F, f)

    def over_fsdp(step):
        def one(i, _):
            step(i)
            return 0

        lax.fori_loop(1, F, one, 0)

    def dcopy(i, who):
        return rep_copy(dmod_ref, drecv.at[who], ds_sem.at[i], dr_sem.at[who], lax.rem(r + i, R))

    for i in range(1, R):
        dcopy(i, r).start()
    sel[...] = jnp.where(iota((D // 8, D), 1) // 8 == iota((D // 8, D), 0), 1.0, 0.0).astype(BF16)
    flat[...] = jnp.zeros_like(flat)
    keep = iota((LANE, D), 0) // RANK == iota((LANE, D), 1) % 8

    def a_rows(x):
        n = x.shape[1]
        return mm_t(sel[:n // 8, :n], low(jnp.where(keep[:, :n], jnp.concatenate([x] * 8, axis=0), 0.0)))

    def put_cols(j, x):
        nb = PAIRS[j][1] // LANE
        for c in range(nb):
            flat[pl.ds(lay.flat_row[2 * j + 1] + c, RANK, stride=nb), :] = x[:, c * LANE:(c + 1) * LANE]

    def place_hidden(ref):
        wide[...] = jnp.zeros_like(wide)
        for k in range(R):
            @pl.when(r == k)
            def _():
                for i in range(F):
                    start = i * (FF // F) + k * fw
                    wide[:, start:start + fw] = ref[:, i * fw:(i + 1) * fw]

    for j, ref in ((1, da1_ref), (2, da2_ref), (3, da3_ref)):
        flat[lay.flat_row[2 * j]:lay.flat_row[2 * j] + D // 8, :] = a_rows(ref[...])
    if fw % 8 == 0:
        y4 = a_rows(da4_ref[...])
        for k in range(R):
            @pl.when(r == k)
            def _():
                for i in range(F):
                    at = lay.flat_row[8] + (i * (FF // F) + k * fw) // 8
                    flat[at:at + fw // 8, :] = y4[i * fw // 8:(i + 1) * fw // 8, :]
    else:
        place_hidden(da4_ref)
        for b in range(FF // D):
            at = lay.flat_row[8] + b * D // 8
            flat[at:at + D // 8, :] = a_rows(wide[:, b * D:(b + 1) * D])
    put_cols(2, db2_ref)
    put_cols(4, db4_ref)
    wide[...] = jnp.zeros_like(wide)
    for k in range(R):
        @pl.when(r == k)
        def _():
            for j in range(3):
                wide[:, j * D + k * cw:j * D + (k + 1) * cw] = db1_ref[:, j * cw:(j + 1) * cw]
    put_cols(1, wide)
    place_hidden(db3_ref)
    put_cols(3, wide)
    for q in range(Q):
        def pack(s, _):
            psend[q, s] = low(flat[pl.ds((s + early) * UR + q * UQ, UQ), :])
            return 0

        lax.fori_loop(0, ns, pack, 0)

    def pcopy(q, who):
        return rep_copy(psend.at[q], precv.at[who], ps_sem.at[q], pr_sem.at[who], q)

    for q in range(Q):
        @pl.when(r != q)
        def _():
            pcopy(q, r).start()
    for i in range(1, R):
        dcopy(i, lax.rem(r + i, R)).wait_recv()
    drecv[r] = dmod_ref[...]
    total = drecv[0]
    for p in range(1, R):
        total = total + drecv[p]
    dall[f] = total

    def gcopy(i, who):
        return fsdp_copy(dall.at[f], dall.at[who], gs_sem.at[i], gr_sem.at[who], lax.rem(f + i, F))

    over_fsdp(lambda i: gcopy(i, f).start())
    du0 = jnp.zeros((RANK, 1), F32)
    u0c = u0c_ref[...]
    for j in range(6):
        row = total[j:j + 1, :]
        du0 = du0 + jnp.sum(b0_ref[:, j * D:(j + 1) * D] * row, axis=1, keepdims=True)
    du0 = 2.0 * du0
    nb = 6 * D // LANE
    for c in range(nb):
        j, k = c // (D // LANE), c % (D // LANE)
        flat[pl.ds(lay.flat_row[1] + c, RANK, stride=nb), :] = 2.0 * u0c * total[j:j + 1, k * LANE:(k + 1) * LANE]
    flat[0:D // 8, :] = a_rows(du0 * low(cond * sig).astype(F32))
    @pl.when(r < Q)
    def _():
        precv[r] = psend[jnp.minimum(r, Q - 1)]

        def pack(s, _):
            hs[s] = low(flat[pl.ds(s * UR + r * UQ, UQ), :])
            return 0

        lax.fori_loop(0, early, pack, 0)
        for p in range(R):
            @pl.when(r != p)
            def _():
                pcopy(r, p).wait_recv()

        def add(s, _):
            total = precv[0, s].astype(F32)
            for p in range(1, R):
                total = total + precv[p, s].astype(F32)
            hs[early + s] = low(total)
            return 0

        lax.fori_loop(0, ns, add, 0)

        def ocopy(owner, who):
            n = lay.hi[owner] - lay.lo[owner]
            return fsdp_copy(hs.at[pl.ds(lay.lo[owner], n)], orecv.at[who, pl.ds(0, n)], os_sem.at[owner], or_sem.at[who], owner)

        for owner in range(F):
            @pl.when(f != owner)
            def _():
                ocopy(owner, f).start()
        for owner in range(F):
            @pl.when(f == owner)
            def _():
                n = lay.hi[owner] - lay.lo[owner]
                orecv[owner, :n] = hs[lay.lo[owner]:lay.hi[owner]]
                for l in range(F):
                    if l != owner:
                        ocopy(owner, l).wait_recv()
        lo = lay.low_of(f)

        def gather_unit(u, _):
            j, a, s = lay.find(f * UNIT_COUNT + u)

            def each(l, total):
                hit = idx_ref[l, pl.ds(1 + j, 1), :][:, :LANE] == a.astype(F32)
                return total + jnp.where(hit, orecv[l, s - lo].astype(F32), 0.0)

            gall[r, u] = low(lax.fori_loop(0, F, each, jnp.zeros((UQ, LANE), F32)))
            return 0

        lax.fori_loop(0, UNIT_COUNT, gather_unit, 0)
        for owner in range(F):
            @pl.when(f != owner)
            def _():
                ocopy(owner, f).wait_send()

    def acopy(i, who):
        return rep_copy(gall.at[r], gall.at[who], as_sem.at[i], ar_sem.at[who], lax.rem(r + i, R))

    @pl.when(r < Q)
    def _():
        for i in range(1, R):
            acopy(i, r).start()
    over_fsdp(lambda i: gcopy(i, lax.rem(f + i, F)).wait_recv())
    dcs = jnp.zeros((2 * F, rows), F32)
    for j in range(6):
        x = jnp.concatenate([dall[l, j:j + 1, :] for l in range(F)], axis=0)
        hi = low(x)
        x = jnp.concatenate([hi, low(x - hi.astype(F32))], axis=0)
        dcs = dcs + mm_t(x, wmod_ref[:, j * D:(j + 1) * D])
    dcs = dcs[:F] + dcs[F:]
    for l in range(F):
        csend[l, 0:1, :rows] = dcs[l:l + 1, :]

    def ccopy(i, who):
        peer = lax.rem(f + i, F)
        return fsdp_copy(csend.at[peer], crecv.at[who], cs_sem.at[i], cr_sem.at[who], peer)

    over_fsdp(lambda i: ccopy(i, f).start())
    crecv[f] = csend[f]
    du0t = jnp.broadcast_to(jnp.concatenate([du0] * 8, axis=0), (LANE, LANE)).T[0:8, :]
    hi = low(du0t)
    extra = (mm_t(hi, z0_ref[...]) + mm_t(low(du0t - hi.astype(F32)), z0_ref[...]))[0:1, :]
    over_fsdp(lambda i: ccopy(i, lax.rem(f + i, F)).wait_recv())
    for l in range(F):
        dcs_ref[0:1, l * rows:(l + 1) * rows] = crecv[l, 0:1, :rows] + extra[:, l * rows:(l + 1) * rows]
    dcs_ref[...] = dcs_ref[...] * slope
    for q in range(Q):
        @pl.when(r != q)
        def _():
            acopy(lax.rem(q - r + R, R), q).wait_recv()

        def unpack(u, _):
            grad_ref[pl.ds(u * UR + q * UQ, UQ), :] = gall[q, u].astype(F32)
            return 0

        lax.fori_loop(0, UNIT_COUNT, unpack, 0)
    for i in range(1, R):
        dcopy(i, r).wait_send()
    for q in range(Q):
        @pl.when(r != q)
        def _():
            pcopy(q, r).wait_send()
    over_fsdp(lambda i: gcopy(i, f).wait_send())
    over_fsdp(lambda i: ccopy(i, f).wait_send())

    @pl.when(r < Q)
    def _():
        for i in range(1, R):
            acopy(i, r).wait_send()


def sds(shape, dtype):
    return jax.ShapeDtypeStruct(shape, dtype)


def dma(n):
    return pltpu.SemaphoreType.DMA((n,))


def call(body, cid, out_shape, scratch, *args, smem=(), hbm=()):
    vm = pl.BlockSpec(memory_space=pltpu.VMEM)
    specs = [vm] * len(args)
    for i in smem:
        specs[i] = pl.BlockSpec(memory_space=pltpu.SMEM)
    for i in hbm:
        specs[i] = pl.BlockSpec(memory_space=pl.ANY)
    params = dict(vmem_limit_bytes=67043328)
    if cid is not None:
        params.update(collective_id=cid, has_side_effects=True)
    return pl.pallas_call(body, out_shape=out_shape, in_specs=specs, out_specs=[vm] * len(out_shape),
                          scratch_shapes=scratch, compiler_params=pltpu.CompilerParams(**params))(*args)


def shards(latents, condition, adapter_index, weight_mod, weight_qkv, weight_proj, weight_fc1, weight_fc2,
           master, moment1, moment2, cotangent):
    R = lax.axis_size("rep")
    F = lax.axis_size("fsdp")
    T = latents.shape[1]
    L = T * R
    hl = HEADS // R
    cw = hl * HEAD_DIM
    fw = FF // (F * R)
    rows = weight_qkv.shape[0]
    scale = HEAD_DIM ** -0.5
    lay = Layout(F)
    UR, UQ, C, NS = lay.rows, lay.part, lay.most, lay.slots
    FW = F * fw
    W3 = 3 * hl * LANE
    SR = UNIT_COUNT * UR
    V = pltpu.VMEM

    shapes = [sds((rows, 3 * cw), BF16), sds((rows, FW), BF16)]
    if fw % 16 == 0:
        wqs, w1s, w2s = call(functools.partial(slice_kernel, R, F), None, shapes + [sds((fw, D), BF16)], [],
                             weight_qkv, weight_fc1, weight_fc2)
    else:
        wqs, w1s = call(lambda q, a, qo, ao: slice_kernel(R, F, q, a, None, qo, ao, None), None, shapes, [],
                        weight_qkv, weight_fc1)
        w2s = lax.dynamic_index_in_dim(weight_fc2.reshape(R, fw, D), lax.axis_index("rep"), 0, keepdims=False)
    grads = [sds((RANK, n), F32) for n in (D, FW, FW, D, D, D, D, 3 * cw)]
    idx, u0c, b0, z0, out, lg, dmod, dA3, dB3, dA4, dB4, dA2, dB2, dA1, dB1 = call(
        functools.partial(step_kernel, R, lay, hl, scale), 4,
        [sds((F, 8, 2 * LANE), F32), sds((RANK, LANE), F32), sds((RANK, 6 * D), F32), sds((D, LANE), BF16),
         sds((T, D), BF16), sds((T, D), F32), sds((8, D), F32)] + grads,
        [V((8, D), F32), V((D, LANE), BF16), V((LANE, 3 * cw), BF16), V((D, LANE), BF16), V((LANE, D), BF16),
         V((D, LANE), BF16), V((LANE, FW), BF16), V((FW, LANE), BF16), V((LANE, D), BF16),
         V((F, rows, 3 * cw), BF16), V((F, rows, D), BF16), V((F, rows, FW), BF16), V((F, fw, D), BF16),
         V((L, D), BF16), V((L, LANE), BF16), V((L, W3), BF16), V((hl * 8, L), F32), V((T, D), BF16),
         V((T, LANE), BF16), V((T, D), F32), V((L, D), BF16),
         V((L, D), BF16), V((F, 8, 2 * LANE), F32), V((hl * LANE, L), BF16), V((hl, T, LANE), F32),
         V((L, cw), BF16), V((R, T, cw), BF16), V((F, C, UQ, LANE), BF16),
         V((R, NS, UQ, LANE), BF16), V((F, 8, D), F32),
         V((L, D), BF16), V((R - 1, T, D), BF16), V((T, D), F32), V((L, D), BF16), V((R - 1, T, D), BF16), V((T, D), F32),
         V((R, T, cw), BF16)]
        + [dma(2)] + [dma(R)] * 2 + [dma(F)] * 6 + [dma(R)] * 2
        + [pltpu.SemaphoreType.DMA((6, F))] * 4 + [dma(R)] * 14,
        latents[0], cotangent[0], condition, adapter_index, weight_mod, master.reshape(SR, LANE), wqs, weight_proj, w1s, w2s,
        smem=(3,), hbm=(4, 5))
    dcond, grad = call(
        functools.partial(tail_kernel, R, lay, hl), 5,
        [sds((1, D), F32), sds((SR, LANE), F32)],
        [V((D // 8, D), BF16), V((NS * UR, LANE), F32), V((RANK, FF), F32),
         V((PARTS, NS - lay.slot[2], UQ, LANE), BF16), V((R, NS - lay.slot[2], UQ, LANE), BF16),
         V((NS, UQ, LANE), BF16), V((F, C, UQ, LANE), BF16), V((R, UNIT_COUNT, UQ, LANE), BF16),
         V((R, 8, D), F32), V((F, 8, D), F32), V((F, 8, 2 * LANE), F32), V((F, 8, 2 * LANE), F32)]
        + [dma(R)] * 2 + [dma(PARTS), dma(R)] + [dma(F)] * 2 + [dma(R)] * 2 + [dma(F)] * 4,
        dmod, dA1, dB1, dA2, dB2, dA3, dB3, dA4, dB4, idx, condition, u0c, b0, z0, weight_mod)
    grad = grad.reshape(-1)
    nm1 = 0.5 * moment1 + 0.5 * grad
    nm2 = 0.5 * moment2 + 0.5 * grad * grad
    corr = 1.0 - 0.5 ** STEP
    nm = master - 0.01 * ((nm1 / corr) / (jnp.sqrt(nm2 / corr) + 1e-08) + 0.1 * master)
    nml = nm.astype(BF16)
    return (out[None], lg[None], dcond, nm, nm1, nm2, nml)


def solution(mesh):
    tok = P("fsdp", "rep", None)
    row = P("fsdp", None)
    vec = P("fsdp")
    return jax.shard_map(shards, mesh=mesh,
                         in_specs=(tok, row, row, row, row, row, row, row, vec, vec, vec, tok),
                         out_specs=(tok, tok, row, vec, vec, vec, vec), check_vma=False)
```
